32 devices in a mesh: lat: 16 (over z, x, core), wave: 2 (over y).
Axes of the slice: x: 2, y: 2, z: 4, core: 2. Of those that a mesh axis runs over, the one named last changes fastest.
Arguments:
- spectrum: float32 [32, 200, 2, 401], P('lat', 'wave'), may hold values from -0.0390625 to 0.0390625
- grad_grid: float32 [128, 32, 5120], P('lat', 'wave'), may hold values from -0.01953125 to 0.01953125
- row_length: int32 [128], P('lat'), may hold values from 2560 to 5120, as said below
- pair_of_slot: int32 [200], replicated, may hold values from 0 to 199, each once
Outputs:
- grid_field: float32 [128, 32, 5120], P('lat', 'wave')
- spectrum_grad: float32 [32, 200, 2, 401], P('lat', 'wave')
The draws below stay inside these ranges and needn't reach their ends.
Inputs may be any that keep to these rules, and one draw needn't show every extreme that they name: `row_length`: every entry is a multiple of 4.
All inputs are finite; a program needn't handle non-finite values.
Results may differ from the reference program's by a relative error of at most 0.0003.
Values sent between devices are 32-bit elements; how exact they have to be, the bound alone decides.
No kernel may reach another device: no remote copies, remote signals or barrier semaphores. Data moves between devices by JAX's collectives and lax.ppermute only.
A program may use at most 128 MiB of HBM per device.

```python
import math
import jax
import jax.numpy as jnp
from jax import lax

TRUNC = 399
NLON = 5120
GRID_LATS = 2560
PAIRS = 200
SLOTS = 401
ROWS = 128
FIELDS = 32


def draw_row_length(key, part):
    quarters = jax.random.randint(key, (ROWS,), NLON // 8, NLON // 4 + 1)
    spots = jax.random.permutation(jax.random.fold_in(key, 7), ROWS)
    places = jnp.arange(ROWS, dtype=jnp.int32)
    quarters = jnp.where(places == spots[0], NLON // 8, quarters)
    quarters = jnp.where(places == spots[1], NLON // 4, quarters)
    return (quarters * 4).astype(jnp.int32)


def levels(own_key, extent, shards, least, largest):
    level = 1.0
    for dim, blocks in shards:
        steps = jax.random.uniform(jax.random.fold_in(jax.random.fold_in(own_key, 6), dim), (blocks,), jnp.float32, least / len(shards), largest / len(shards))
        level = level * jnp.repeat(jnp.exp(steps), extent[dim] // blocks).reshape((-1,) + (1,) * (len(extent) - 1 - dim))
    return level


def scatter_about(stream_key, extent, width, most, pieces=(), kind=jnp.bfloat16):
    loudness = levels(stream_key, extent, pieces, -0.22, 0.18) if pieces else 1.0
    values = jax.random.normal(stream_key, extent, jnp.float32) * width * loudness
    return jnp.minimum(jnp.maximum(values, -most), most).astype(kind)


def setup_inputs(seed: int = 0) -> dict:
    keys = jax.random.split(jax.random.key(seed), 5)
    return {
        "spectrum": scatter_about(keys[0], (FIELDS, PAIRS, 2, SLOTS), (1.0 / (TRUNC + 1)), 0.0390625, ((0, 16), (1, 2)), jnp.float32),
        "grad_grid": scatter_about(keys[1], (ROWS, FIELDS, NLON), ((NLON * ROWS) ** -0.5), 0.01953125, ((0, 16), (1, 2)), jnp.float32),
        "row_length": draw_row_length(jax.random.fold_in(keys[4], 71), 0),
        "pair_of_slot": jax.random.permutation(keys[3], PAIRS).astype(jnp.int32),
    }


highest = lax.Precision.HIGHEST

def colatitudes(first_row, row_total, window_total):
    offsets = jnp.arange(row_total, dtype=jnp.float32) + (first_row + 0.5 - window_total / 2.0)
    return math.pi / 2.0 + offsets * (math.pi / GRID_LATS)

def member_table(pair_ids, colatitude):
    cosine = jnp.cos(colatitude)[None, :]
    sine_row = jnp.sin(colatitude)[None, :]
    low_order = pair_ids.astype(jnp.float32)[:, None]
    high_order = (TRUNC - pair_ids).astype(jnp.float32)[:, None]
    boundary = (TRUNC + 1 - pair_ids).astype(jnp.int32)[:, None]
    gamma_half = lax.lgamma(jnp.float32(1.5))

    def diagonal(orders):
        return jnp.exp(0.5 * (lax.lgamma(orders + 1.5) - gamma_half - lax.lgamma(orders + 1.0)) + orders * jnp.log(sine_row))
    start_low = diagonal(low_order)
    start_high = diagonal(high_order)

    def advance(carry, unused):
        earlier, latest, position = carry
        is_upper = position >= boundary
        wave_number = jnp.where(is_upper, high_order, low_order)
        offset_n = jnp.where(is_upper, position - boundary, position)
        degree = wave_number + offset_n.astype(jnp.float32)
        forward = jnp.sqrt((4.0 * degree * degree - 1.0) / jnp.maximum(degree * degree - wave_number * wave_number, 1.0))
        lower_deg = degree - 1.0
        backward = jnp.sqrt(jnp.maximum(4.0 * lower_deg * lower_deg - 1.0, 1.0) / jnp.maximum(lower_deg * lower_deg - wave_number * wave_number, 1.0))
        recurred = forward * (cosine * latest - earlier / backward)
        second_value = jnp.sqrt(2.0 * wave_number + 3.0) * cosine * latest
        result = jnp.where(offset_n == 0, jnp.where(is_upper, start_high, start_low), jnp.where(offset_n == 1, second_value, recurred))
        return ((latest, result, position + 1), result)
    blank = jnp.zeros((pair_ids.shape[0], colatitude.shape[0]), jnp.float32)
    start_state = (blank, blank, jnp.zeros((), jnp.int32))
    final_state, columns = lax.scan(advance, start_state, None, length=TRUNC + 2, unroll=16)
    columns = jnp.transpose(columns, (1, 0, 2))
    positions = jnp.arange(TRUNC + 2, dtype=jnp.int32)[None, :]
    in_upper = (positions >= boundary)[:, :, None]
    return jnp.stack([jnp.where(in_upper, 0.0, columns), jnp.where(in_upper, columns, 0.0)], axis=1)

def reference(spectrum, grad_grid, row_length, pair_of_slot):
    table = member_table(pair_of_slot, colatitudes(0, ROWS, ROWS))
    fourier = jnp.einsum('fsri,scil->lfrcs', spectrum, table, precision=highest)
    numbers = jnp.concatenate([pair_of_slot, TRUNC - pair_of_slot]).astype(jnp.int32)
    weights = jnp.where(numbers == 0, 1.0, 2.0).astype(jnp.float32)
    coeffs = fourier.reshape(ROWS, FIELDS, 2, 2 * PAIRS)

    def per_row(items):
        coeff_row, grad_row, length = items
        points = jnp.arange(NLON, dtype=jnp.int32)
        phase = numbers[:, None] * points[None, :] % length
        angle = phase.astype(jnp.float32) * (2.0 * math.pi / length.astype(jnp.float32))
        cosines = jnp.cos(angle)
        sines = jnp.sin(angle)
        real_part = weights * coeff_row[:, 0]
        imag_part = weights * coeff_row[:, 1]
        grid_row = jnp.dot(real_part, cosines, precision=highest, preferred_element_type=jnp.float32) - jnp.dot(imag_part, sines, precision=highest, preferred_element_type=jnp.float32)
        inside = (points < length)[None, :]
        grid_row = jnp.where(inside, grid_row, 0.0)
        masked = jnp.where(inside, grad_row, 0.0)
        cos_sum = jnp.dot(masked, cosines.T, precision=highest, preferred_element_type=jnp.float32)
        sin_sum = jnp.dot(masked, sines.T, precision=highest, preferred_element_type=jnp.float32)
        return (grid_row, jnp.stack([weights * cos_sum, -weights * sin_sum], axis=1))
    grid_field, fourier_grad = lax.map(per_row, (coeffs, grad_grid, row_length))
    fourier_grad = fourier_grad.reshape(ROWS, FIELDS, 2, 2, PAIRS)
    spectrum_grad = jnp.einsum('scil,lfrcs->fsri', table, fourier_grad, precision=highest)
    return (grid_field, spectrum_grad)
```

```python
import math

import jax
import jax.numpy as jnp
import numpy as np
from jax import lax
from jax.experimental import pallas as pl
from jax.experimental.pallas import tpu as pltpu
from jax.sharding import PartitionSpec as P

GRID_LATS = 2560
LANES = 128
BLOCK = 256
SUB = 16
UNROLL = 8
GROUP = 2
VMEM_LIMIT = 56 * 1024 * 1024


def fit_trig():
    nodes = np.cos(np.pi * (np.arange(400) + 0.5) / 400)
    y = 0.125 * (nodes + 1.0) * 1.01
    u = np.sqrt(y)
    sin_fit = np.polynomial.chebyshev.Chebyshev.fit(y, np.sin(2 * np.pi * u) / u, 7, domain=[0, 0.2525])
    cos_fit = np.polynomial.chebyshev.Chebyshev.fit(y, np.cos(2 * np.pi * u), 8, domain=[0, 0.2525])
    to_power = lambda fit: [float(c) for c in fit.convert(kind=np.polynomial.Polynomial).coef]
    return to_power(sin_fit), to_power(cos_fit)


SIN_COEF, COS_COEF = fit_trig()


def horner(coefs, y):
    value = jnp.full_like(y, coefs[-1])
    for c in coefs[-2::-1]:
        value = value * y + c
    return value


def cos_sin(product, length, inverse):
    turns = jnp.floor(product * inverse + 0.5)
    u = (product - turns * length) * inverse
    y = u * u
    return horner(COS_COEF, y), u * horner(SIN_COEF, y)


def split(value):
    high = value.astype(jnp.bfloat16)
    low = (value - high.astype(jnp.float32)).astype(jnp.bfloat16)
    return high, low


def legendre_step(i, latest, earlier, coef_ref, cosines, tops, boundary):
    forward = coef_ref[i, 0:1, :]
    backward = coef_ref[i, 1:2, :]
    out = []
    for g in range(len(latest)):
        value = (forward * cosines[g]) * latest[g] - backward * earlier[g]
        if tops is not None:
            value = jnp.where(boundary == i, tops[g], value)
        out.append(value)
    return out


def starts(first_ref, geometry_ref, rows):
    log_sine = geometry_ref[1, rows, :]
    low = jnp.exp(first_ref[0:1, :] + first_ref[2:3, :] * log_sine)
    high = jnp.exp(first_ref[1:2, :] + first_ref[3:4, :] * log_sine)
    return low, high


def synthesis_kernel(slots, low_ref, high_ref, coef_ref, first_ref, geometry_ref, bound_ref, out_ref):
    combos = low_ref.shape[1]
    half = out_ref.shape[0] // 2
    head = slots // 2 // UNROLL * UNROLL
    boundary = bound_ref[0:1, :]
    sign = bound_ref[1:2, :].astype(jnp.float32)

    def one_group(step, carry):
        del carry
        index = [step * GROUP + k for k in range(GROUP)]
        rows = [pl.ds(pl.multiple_of(g * 8, 8), 8) for g in index]
        cosines = [geometry_ref[0, r, :] for r in rows]
        lows, tops = zip(*[starts(first_ref, geometry_ref, r) for r in rows])
        zero = jnp.zeros((8, LANES), jnp.float32)
        latest = [zero] * GROUP
        earlier = [-v for v in lows]

        def accumulate(sums, values, source, i):
            out = list(sums)
            for j in range(combos):
                weight = source[i, j : j + 1, :]
                for g in range(GROUP):
                    k = j * GROUP + g
                    out[k] = out[k] + weight * values[g]
            return out

        def head_steps(it, state):
            latest, earlier, even, odd = state
            for u in range(UNROLL):
                i = it * UNROLL + u
                value = legendre_step(i, latest, earlier, coef_ref, cosines, None, boundary)
                earlier, latest = latest, value
                if u % 2 == 0:
                    even = accumulate(even, value, low_ref, i)
                else:
                    odd = accumulate(odd, value, low_ref, i)
            return latest, earlier, even, odd

        def tail_step(i, parity, state):
            latest, earlier, even, odd, even_up, odd_up = state
            value = legendre_step(i, latest, earlier, coef_ref, cosines, tops, boundary)
            earlier, latest = latest, value
            if parity == 0:
                even = accumulate(even, value, low_ref, i)
                even_up = accumulate(even_up, value, high_ref, i - head)
            else:
                odd = accumulate(odd, value, low_ref, i)
                odd_up = accumulate(odd_up, value, high_ref, i - head)
            return latest, earlier, even, odd, even_up, odd_up

        def tail_steps(it, state):
            for u in range(UNROLL):
                state = tail_step(head + it * UNROLL + u, u % 2, state)
            return state

        blank = [zero] * (combos * GROUP)
        latest, earlier, even, odd = lax.fori_loop(0, head // UNROLL, head_steps, (latest, earlier, blank, blank))
        whole = (slots - head) // UNROLL
        state = lax.fori_loop(0, whole, tail_steps, (latest, earlier, even, odd, blank, blank))
        for i in range(head + whole * UNROLL, slots):
            state = tail_step(i, i % 2, state)
        even, odd, even_up, odd_up = state[2:]
        for j in range(combos):
            for g in range(GROUP):
                k = j * GROUP + g
                mirror = 2 * half - 1 - index[g]
                out_ref[index[g], j, 0] = even[k] + odd[k]
                out_ref[mirror, j, 0] = even[k] - odd[k]
                out_ref[index[g], j, 1] = even_up[k] + odd_up[k]
                out_ref[mirror, j, 1] = sign * (even_up[k] - odd_up[k])
        return 0

    lax.fori_loop(0, half // GROUP, one_group, 0)


def truncation_kernel(slots, grad_ref, coef_ref, first_ref, geometry_ref, bound_ref, out_ref, sum_ref):
    combos = grad_ref.shape[1]
    half = grad_ref.shape[0] // 2
    head = slots // 2 // UNROLL * UNROLL
    boundary = bound_ref[0:1, :]
    sign = bound_ref[1:2, :].astype(jnp.float32)
    sum_ref[...] = jnp.zeros_like(sum_ref)

    def one_group(step, carry):
        del carry
        index = [step * GROUP + k for k in range(GROUP)]
        rows = [pl.ds(pl.multiple_of(g * 8, 8), 8) for g in index]
        cosines = [geometry_ref[0, r, :] for r in rows]
        lows, tops = zip(*[starts(first_ref, geometry_ref, r) for r in rows])
        zero = jnp.zeros((8, LANES), jnp.float32)
        fields = {}
        for j in range(combos):
            for g in range(GROUP):
                mirror = 2 * half - 1 - index[g]
                for c in range(2):
                    here = grad_ref[index[g], j, c]
                    there = grad_ref[mirror, j, c]
                    if c == 1:
                        there = sign * there
                    fields[0, c, j, g] = here + there
                    fields[1, c, j, g] = here - there

        def add(i, parity, value, split_members):
            upper = boundary <= i
            for j in range(combos):
                total = None
                for g in range(GROUP):
                    field = fields[parity, 0, j, g]
                    if split_members:
                        field = jnp.where(upper, fields[parity, 1, j, g], field)
                    term = field * value[g]
                    total = term if total is None else total + term
                sum_ref[i, j] = sum_ref[i, j] + total

        def head_steps(it, state):
            latest, earlier = state
            for u in range(UNROLL):
                i = it * UNROLL + u
                value = legendre_step(i, latest, earlier, coef_ref, cosines, None, boundary)
                earlier, latest = latest, value
                add(i, u % 2, value, False)
            return latest, earlier

        def tail_step(i, parity, state):
            latest, earlier = state
            value = legendre_step(i, latest, earlier, coef_ref, cosines, tops, boundary)
            add(i, parity, value, True)
            return value, latest

        def tail_steps(it, state):
            for u in range(UNROLL):
                state = tail_step(head + it * UNROLL + u, u % 2, state)
            return state

        state = lax.fori_loop(0, head // UNROLL, head_steps, ([zero] * GROUP, [-v for v in lows]))
        whole = (slots - head) // UNROLL
        state = lax.fori_loop(0, whole, tail_steps, state)
        for i in range(head + whole * UNROLL, slots):
            state = tail_step(i, i % 2, state)
        return 0

    lax.fori_loop(0, half // GROUP, one_group, 0)
    out_ref[...] = jnp.sum(sum_ref[...], axis=2)


def legendre_inputs(pairs, slots, window_rows):
    trunc = slots - 2
    angle = (np.arange(window_rows // 2) + 0.5 - window_rows / 2.0) * (math.pi / GRID_LATS)
    geometry = np.stack([-np.sin(angle), np.log(np.cos(angle))]).astype(np.float32)
    geometry = jnp.asarray(np.broadcast_to(geometry[:, :, None], geometry.shape + (LANES,)))
    orders = jnp.stack([pairs, trunc - pairs]).astype(jnp.float32)
    gamma_half = lax.lgamma(jnp.float32(1.5))
    first = 0.5 * (lax.lgamma(orders + 1.5) - gamma_half - lax.lgamma(orders + 1.0))
    first = jnp.concatenate([first, orders], axis=0)
    boundary = (trunc + 1 - pairs)[None, :]
    sign = jnp.where(boundary % 2 == 0, 1, -1)
    bound = jnp.concatenate([boundary, sign], axis=0).astype(jnp.int32)
    position = jnp.arange(slots, dtype=jnp.int32)[:, None]
    upper = position >= boundary
    order = jnp.where(upper, orders[1:2], orders[0:1])
    offset = jnp.where(upper, position - boundary, position)
    degree = order + offset.astype(jnp.float32)
    forward_square = (4.0 * degree * degree - 1.0) / jnp.maximum(degree * degree - order * order, 1.0)
    lower = degree - 1.0
    backward_square = jnp.maximum(4.0 * lower * lower - 1.0, 1.0) / jnp.maximum(lower * lower - order * order, 1.0)
    forward = jnp.sqrt(jnp.maximum(forward_square, 0.0))
    ratio = forward / jnp.sqrt(backward_square)
    forward = jnp.where(position == 0, 0.0, forward)
    backward = jnp.where(position == 0, 1.0, jnp.where(offset <= 1, 0.0, ratio))
    coef = jnp.stack([forward, backward], axis=1)
    return coef, first, geometry, bound, upper


def synthesis(spectrum, tables):
    fields, pair_dev, _, slots = spectrum.shape
    coef, first, geometry, bound, upper = tables
    lat = geometry.shape[1] * 2 // 8
    combos = fields * 2
    head = slots // 2 // UNROLL * UNROLL
    turned = jnp.transpose(spectrum, (3, 0, 2, 1)).reshape(slots, combos, pair_dev)
    turned = jnp.pad(turned, ((0, 0), (0, 0), (0, LANES - pair_dev)))
    low = jnp.where(upper[:, None, :], 0.0, turned)
    high = jnp.where(upper[:, None, :], turned, 0.0)[head:]
    return pl.pallas_call(
        lambda *refs: synthesis_kernel(slots, *refs),
        out_shape=jax.ShapeDtypeStruct((lat, combos, 2, 8, LANES), jnp.float32),
        compiler_params=pltpu.CompilerParams(vmem_limit_bytes=VMEM_LIMIT),
        cost_estimate=pl.CostEstimate(flops=10**10, bytes_accessed=10**6, transcendentals=0),
        name="synthesis",
    )(low, high, coef, first, geometry, bound)


def truncation(grad, tables, slots):
    coef, first, geometry, bound, _ = tables
    combos = grad.shape[1]
    return pl.pallas_call(
        lambda *refs: truncation_kernel(slots, *refs),
        out_shape=jax.ShapeDtypeStruct((slots, combos, LANES), jnp.float32),
        scratch_shapes=[pltpu.VMEM((slots, combos, 8, LANES), jnp.float32)],
        compiler_params=pltpu.CompilerParams(vmem_limit_bytes=VMEM_LIMIT),
        cost_estimate=pl.CostEstimate(flops=10**10, bytes_accessed=10**6, transcendentals=0),
        name="truncation",
    )(grad, coef, first, geometry, bound)


def wave_rows(wave_ref, trunc):
    pair = wave_ref[0:1, :]
    is_even = pair % 2 == 0
    even = jnp.where(is_even, pair, trunc - pair)
    return is_even, even.astype(jnp.float32), (trunc - even).astype(jnp.float32)


def row_tables(even, odd, length, inverse, table_refs):
    lanes = even.shape[1]
    steps = lax.broadcasted_iota(jnp.int32, (SUB, lanes), 0).astype(jnp.float32)
    for number, high_ref, low_ref in ((even, *table_refs[:2]), (odd, *table_refs[2:])):
        near_cos, near_sin = cos_sin(steps * number, length, inverse)
        far_cos, far_sin = cos_sin(steps * (number * SUB), length, inverse)
        for a in range(BLOCK // SUB):
            turn_cos = far_cos[a : a + 1, :]
            turn_sin = far_sin[a : a + 1, :]
            rows = pl.ds(a * SUB, SUB)
            high, low = split(near_cos * turn_cos - near_sin * turn_sin)
            high_ref[rows, :lanes] = high
            low_ref[rows, :lanes] = low
            high, low = split(near_sin * turn_cos + near_cos * turn_sin)
            high_ref[rows, lanes:] = high
            low_ref[rows, lanes:] = low


def outer_turns(number, blocks, length, inverse):
    steps = lax.broadcasted_iota(jnp.int32, (SUB * -(-blocks // SUB), number.shape[1]), 0).astype(jnp.float32)
    return cos_sin(steps * (number * BLOCK), length, inverse)


def three_pass(left_high, left_low, right_high, right_low, dims):
    dot = lambda a, b: lax.dot_general(a, b, (dims, ((), ())), preferred_element_type=jnp.float32)
    return dot(left_high, right_high) + (dot(left_low, right_high) + dot(left_high, right_low))


def row_kernel(parts, trunc, order_ref, length_ref, *refs):
    part_refs = refs[:parts]
    wave_ref, out_ref = refs[parts : parts + 2]
    table_refs = refs[parts + 2 : parts + 6]
    left_refs = refs[parts + 6 : parts + 10]
    shift_ref, wide_ref = refs[parts + 10 :]
    fields, nlon = out_ref.shape[1:]
    blocks = nlon // 2 // BLOCK
    row = pl.program_id(0)
    source = jnp.where(order_ref[0] == 1, 7 - row, row)
    size = length_ref[row]
    half = size // 2
    length = size.astype(jnp.float32)
    inverse = 1.0 / jnp.full((1, LANES), length)[:, :1]
    is_even, even, odd = wave_rows(wave_ref, trunc)
    row_tables(even, odd, length, inverse, table_refs)

    def coefficients(r, c):
        pieces = []
        for ref in part_refs:
            pieces.append(ref[pl.ds((r * 2 + c) * 8 + source, fields, stride=32), :])
        return jnp.concatenate(pieces, axis=1) if len(pieces) > 1 else pieces[0]

    lanes = even.shape[1]
    member = [[coefficients(r, c) for c in range(2)] for r in range(2)]
    for parity, number in ((0, even), (1, odd)):
        high_ref, low_ref = left_refs[2 * parity : 2 * parity + 2]
        weight = jnp.where(number == 0.0, 1.0, 2.0)
        real, imag = [
            jnp.where(is_even, member[r][parity], member[r][1 - parity]) * weight for r in range(2)
        ]
        turn_cos, turn_sin = outer_turns(number, blocks, length, inverse)
        for b in range(blocks):
            c = turn_cos[b : b + 1, :]
            s = turn_sin[b : b + 1, :]
            rows = pl.ds(b * fields, fields)
            high, low = split(real * c - imag * s)
            high_ref[rows, :lanes] = high
            low_ref[rows, :lanes] = low
            high, low = split(-(real * s + imag * c))
            high_ref[rows, lanes:] = high
            low_ref[rows, lanes:] = low

    dims = ((1,), (1,))
    even_sum = three_pass(left_refs[0][...], left_refs[1][...], table_refs[0][...], table_refs[1][...], dims)
    odd_sum = three_pass(left_refs[2][...], left_refs[3][...], table_refs[2][...], table_refs[3][...], dims)
    first = even_sum + odd_sum
    second = even_sum - odd_sum
    point = lax.broadcasted_iota(jnp.int32, (fields, BLOCK), 1)
    wide_ref[:, blocks * BLOCK :] = jnp.zeros((fields, wide_ref.shape[1] - blocks * BLOCK), jnp.float32)
    shift_ref[:, blocks * BLOCK :] = jnp.zeros((fields, LANES), jnp.float32)
    for b in range(blocks):
        inside = point < half - b * BLOCK
        cols = pl.ds(b * BLOCK, BLOCK)
        wide_ref[:, cols] = jnp.where(inside, first[b * fields : (b + 1) * fields], 0.0)
        shift_ref[:, cols] = jnp.where(inside, second[b * fields : (b + 1) * fields], 0.0)
    moved = pltpu.roll(shift_ref[...], half % LANES, 1)
    window = pl.ds(pl.multiple_of(half // LANES * LANES, LANES), blocks * BLOCK + LANES)
    wide_ref[:, window] = wide_ref[:, window] + moved
    out_ref[0] = wide_ref[:, :nlon]


def adjoint_kernel(parts, trunc, order_ref, length_ref, grad_ref, wave_ref, *refs):
    part_refs = refs[:parts]
    table_refs = refs[parts : parts + 4]
    left_refs = refs[parts + 4 : parts + 8]
    wide_ref = refs[parts + 8]
    fields, nlon = grad_ref.shape[1:]
    blocks = nlon // 2 // BLOCK
    row = pl.program_id(0)
    target = jnp.where(order_ref[0] == 1, 7 - row, row)
    size = length_ref[row]
    half = size // 2
    length = size.astype(jnp.float32)
    inverse = 1.0 / jnp.full((1, LANES), length)[:, :1]
    is_even, even, odd = wave_rows(wave_ref, trunc)
    row_tables(even, odd, length, inverse, table_refs)
    wide_ref[:, :nlon] = grad_ref[0]
    wide_ref[:, nlon:] = jnp.zeros((fields, wide_ref.shape[1] - nlon), jnp.float32)
    span = blocks * BLOCK + LANES
    window = pl.ds(pl.multiple_of(half // LANES * LANES, LANES), span)
    moved = pltpu.roll(wide_ref[:, window], (span - half % LANES) % span, 1)
    point = lax.broadcasted_iota(jnp.int32, (fields, BLOCK), 1)
    for b in range(blocks):
        inside = point < half - b * BLOCK
        cols = slice(b * BLOCK, (b + 1) * BLOCK)
        rows = pl.ds(b * fields, fields)
        first = jnp.where(inside, grad_ref[0, :, cols], 0.0)
        second = jnp.where(inside, moved[:, cols], 0.0)
        left_refs[0][rows, :], left_refs[1][rows, :] = split(first + second)
        left_refs[2][rows, :], left_refs[3][rows, :] = split(first - second)
    dims = ((1,), (0,))
    lanes = even.shape[1]
    result = []
    for parity, number in ((0, even), (1, odd)):
        k = 2 * parity
        folded = three_pass(
            left_refs[k][...], left_refs[k + 1][...], table_refs[k][...], table_refs[k + 1][...], dims
        )
        turn_cos, turn_sin = outer_turns(number, blocks, length, inverse)
        real = imag = 0.0
        for b in range(blocks):
            c = turn_cos[b : b + 1, :]
            s = turn_sin[b : b + 1, :]
            cos_part = folded[b * fields : (b + 1) * fields, :lanes]
            sin_part = folded[b * fields : (b + 1) * fields, lanes:]
            real = real + (c * cos_part - s * sin_part)
            imag = imag - (s * cos_part + c * sin_part)
        weight = jnp.where(number == 0.0, 1.0, 2.0)
        result.append((weight * real, weight * imag))
    for r in range(2):
        for c in range(2):
            value = jnp.where(is_even, result[c][r], result[1 - c][r])
            start = 0
            for ref in part_refs:
                width = ref.shape[1]
                ref[pl.ds((r * 2 + c) * 8 + target, fields, stride=32), :] = value[:, start : start + width]
                start += width


def row_scratch(blocks, fields, lanes, nlon, left_width):
    bf16 = jnp.bfloat16
    tables = [pltpu.VMEM((BLOCK, 2 * lanes), bf16)] * 4
    lefts = [pltpu.VMEM((blocks * fields, left_width), bf16)] * 4
    return tables, lefts


def rows_out(parts, waves, order, row_length, fields, nlon, trunc):
    row_dev = row_length.shape[0]
    lanes = waves.shape[1]
    blocks = nlon // 2 // BLOCK
    tables, lefts = row_scratch(blocks, fields, lanes, nlon, 2 * lanes)
    whole = lambda shape: pl.BlockSpec(shape, lambda i, *_: (0,) * len(shape))
    specs = []
    for part, pick in parts:
        width = part.shape[-1]
        if pick:
            specs.append(pl.BlockSpec((fields * 32, width), lambda i, order, length: (order[1], 0)))
        else:
            specs.append(whole((fields * 32, width)))
    span = blocks * BLOCK + LANES
    return pl.pallas_call(
        lambda *refs: row_kernel(len(parts), trunc, *refs),
        grid_spec=pltpu.PrefetchScalarGridSpec(
            num_scalar_prefetch=2,
            grid=(row_dev,),
            in_specs=specs + [whole(waves.shape)],
            out_specs=pl.BlockSpec((1, fields, nlon), lambda i, *_: (i, 0, 0)),
            scratch_shapes=tables
            + lefts
            + [pltpu.VMEM((fields, span), jnp.float32), pltpu.VMEM((fields, nlon // 2 + span), jnp.float32)],
        ),
        out_shape=jax.ShapeDtypeStruct((row_dev, fields, nlon), jnp.float32),
        compiler_params=pltpu.CompilerParams(vmem_limit_bytes=VMEM_LIMIT),
        cost_estimate=pl.CostEstimate(flops=10**10, bytes_accessed=10**6, transcendentals=0),
        name="rows",
    )(order, row_length, *[p.reshape(-1, p.shape[-1]) for p, _ in parts], waves)


def rows_adjoint(grad_grid, waves, widths, order, row_length, trunc):
    row_dev, fields, nlon = grad_grid.shape
    lanes = waves.shape[1]
    blocks = nlon // 2 // BLOCK
    tables, lefts = row_scratch(blocks, fields, lanes, nlon, BLOCK)
    whole = lambda shape: pl.BlockSpec(shape, lambda i, *_: (0,) * len(shape))
    shapes = [(fields * 32, width) for width in widths]
    span = blocks * BLOCK + LANES
    return pl.pallas_call(
        lambda *refs: adjoint_kernel(len(widths), trunc, *refs),
        grid_spec=pltpu.PrefetchScalarGridSpec(
            num_scalar_prefetch=2,
            grid=(row_dev,),
            in_specs=[pl.BlockSpec((1, fields, nlon), lambda i, *_: (i, 0, 0)), whole(waves.shape)],
            out_specs=[whole(s) for s in shapes],
            scratch_shapes=tables + lefts + [pltpu.VMEM((fields, nlon // 2 + span), jnp.float32)],
        ),
        out_shape=[jax.ShapeDtypeStruct(s, jnp.float32) for s in shapes],
        compiler_params=pltpu.CompilerParams(vmem_limit_bytes=VMEM_LIMIT),
        cost_estimate=pl.CostEstimate(flops=10**10, bytes_accessed=10**6, transcendentals=0),
        name="adjoint",
    )(order, row_length, grad_grid, waves)


def body(spectrum, grad_grid, row_length, pair_of_slot):
    row_dev, grid_fields, nlon = grad_grid.shape
    own_fields, pair_dev, _, slots = spectrum.shape
    trunc = slots - 2
    lat = lax.axis_size("lat")
    wave = lax.axis_size("wave")
    lat_index = lax.axis_index("lat")
    wave_index = lax.axis_index("wave")
    combos = own_fields * 2
    pad = LANES - pair_dev
    own_pairs = jnp.pad(lax.dynamic_slice_in_dim(pair_of_slot, wave_index * pair_dev, pair_dev), (0, pad))
    tables = legendre_inputs(own_pairs, slots, row_dev * lat)
    mirrored = (lat_index >= lat // 2).astype(jnp.int32)
    order = jnp.stack([mirrored, wave_index.astype(jnp.int32)])
    two = wave == 2
    swap = [(0, 1), (1, 0)]
    if two:
        other = lax.dynamic_slice_in_dim(pair_of_slot, (1 - wave_index) * pair_dev, pair_dev)
        waves = jnp.concatenate([own_pairs, jnp.pad(other, (0, pad))])[None, :]
        widths = (LANES, LANES)
    else:
        total = pair_of_slot.shape[0]
        width = -(-total // LANES) * LANES
        waves = jnp.pad(pair_of_slot, (0, width - total))[None, :]
        widths = (LANES,) * (width // LANES)

    coeffs = synthesis(spectrum, tables)
    coeffs = lax.all_to_all(coeffs, "lat", split_axis=0, concat_axis=0, tiled=True)

    folded = rows_adjoint(grad_grid, waves, widths, order, row_length, trunc)
    piece = (lat // wave, combos, 2, 8, LANES)
    if two:
        received = lax.ppermute(folded[1], "wave", swap).reshape(piece)
        mine = folded[0].reshape(piece)
        first = wave_index == 0
        grads = jnp.where(
            first, jnp.concatenate([mine, received], axis=0), jnp.concatenate([received, mine], axis=0)
        )
    else:
        turned = jnp.concatenate(folded, axis=1)[:, : pair_of_slot.shape[0]].reshape(-1, wave, pair_dev)
        turned = jnp.pad(jnp.transpose(turned, (1, 0, 2)), ((0, 0), (0, 0), (0, pad)))
        grads = lax.all_to_all(turned, "wave", split_axis=0, concat_axis=0, tiled=True)
        grads = grads.reshape((lat,) + piece[1:])
    grads = lax.all_to_all(grads, "lat", split_axis=0, concat_axis=0, tiled=True)

    if two:
        outgoing = lax.dynamic_slice_in_dim(coeffs, (1 - wave_index) * (lat // 2), lat // 2)
        incoming = lax.ppermute(outgoing, "wave", swap)
        parts = [(coeffs, True), (incoming, False)]
    else:
        turned = lax.all_to_all(coeffs, "wave", split_axis=0, concat_axis=0, tiled=True)
        turned = turned.reshape(wave, -1, LANES)[:, :, :pair_dev]
        turned = jnp.transpose(turned, (1, 0, 2)).reshape(turned.shape[1], -1)
        turned = jnp.pad(turned, ((0, 0), (0, waves.shape[1] - turned.shape[1])))
        parts = [(turned[:, k : k + LANES], False) for k in range(0, waves.shape[1], LANES)]
    grid_field = rows_out(parts, waves, order, row_length, grid_fields, nlon, trunc)

    turned = truncation(grads, tables, slots)[:, :, :pair_dev]
    turned = turned.reshape(slots, own_fields, 2, pair_dev)
    return grid_field, jnp.transpose(turned, (1, 3, 2, 0))


def solution(mesh):
    placed = (P("lat", "wave", None, None), P("lat", "wave", None), P("lat"), P())
    return jax.shard_map(
        body,
        mesh=mesh,
        in_specs=placed,
        out_specs=(P("lat", "wave", None), P("lat", "wave", None, None)),
        check_vma=False,
    )
```

```python
import math

import jax
import jax.numpy as jnp
import numpy as np
from jax import lax
from jax.experimental import pallas as pl
from jax.experimental.pallas import tpu as pltpu
from jax.sharding import PartitionSpec as P

GRID_LATS = 2560
LANES = 128
BLOCK = 256
SUB = 16
CHUNK = 8
GROUP = 2
VMEM_LIMIT = 56 * 1024 * 1024


def fit_trig():
    nodes = np.cos(np.pi * (np.arange(400) + 0.5) / 400)
    y = 0.125 * (nodes + 1.0) * 1.01
    u = np.sqrt(y)
    sin_fit = np.polynomial.chebyshev.Chebyshev.fit(y, np.sin(2 * np.pi * u) / u, 7, domain=[0, 0.2525])
    cos_fit = np.polynomial.chebyshev.Chebyshev.fit(y, np.cos(2 * np.pi * u), 8, domain=[0, 0.2525])
    to_power = lambda fit: [float(c) for c in fit.convert(kind=np.polynomial.Polynomial).coef]
    return to_power(sin_fit), to_power(cos_fit)


SIN_COEF, COS_COEF = fit_trig()


def horner(coefs, y):
    value = jnp.full_like(y, coefs[-1])
    for c in coefs[-2::-1]:
        value = value * y + c
    return value


def cos_sin(product, length, inverse):
    turns = jnp.floor(product * inverse + 0.5)
    u = (product - turns * length) * inverse
    y = u * u
    return horner(COS_COEF, y), u * horner(SIN_COEF, y)


def split(value):
    high = value.astype(jnp.bfloat16)
    low = (value - high.astype(jnp.float32)).astype(jnp.bfloat16)
    return high, low


def lane_pairs(pairs_ref, wide_ref, kind, share):
    total = pairs_ref.shape[1]
    width = wide_ref.shape[1]
    if kind in ("own", "other"):
        wave = lax.axis_index("wave")
        first = share * (wave if kind == "own" else 1 - wave)
        valid = share
    else:
        first = LANES * kind
        valid = min(LANES, total - first)
    wide_ref[0:1, :total] = pairs_ref[...]
    lanes = pltpu.roll(wide_ref[...], (width - first) % width, 1)[0:1, :LANES]
    return jnp.where(lax.broadcasted_iota(jnp.int32, (1, LANES), 1) < valid, lanes, 0)


def lane_facts(pairs_ref, wide_ref, share, trunc):
    pair = lane_pairs(pairs_ref, wide_ref, "own", share)
    boundary = trunc + 1 - pair
    delay = jnp.bitwise_and(-boundary, CHUNK - 1)
    return pair, delay, boundary + delay


def fill_coefficients(pair, delay, change, trunc, forward_ref, backward_ref):
    low_order = pair.astype(jnp.float32)
    high_order = trunc - low_order

    def fill(chunk, carry):
        step = lax.broadcasted_iota(jnp.int32, (CHUNK, LANES), 0) + chunk * CHUNK
        upper = step >= change
        order = jnp.where(upper, high_order, low_order)
        offset = jnp.where(upper, step - change, step - delay)
        degree = order + offset.astype(jnp.float32)
        lower = degree - 1.0
        top = jnp.maximum(4.0 * degree * degree - 1.0, 1.0)
        base = jnp.maximum(degree * degree - order * order, 1.0)
        lower_top = jnp.maximum(4.0 * lower * lower - 1.0, 1.0)
        lower_base = jnp.maximum(lower * lower - order * order, 1.0)
        forward = jnp.sqrt(top / base)
        backward = jnp.sqrt((top * lower_base) / (base * lower_top))
        rows = pl.ds(pl.multiple_of(chunk * CHUNK, CHUNK), CHUNK)
        forward_ref[rows, :] = jnp.where(offset <= 0, 0.0, forward)
        backward_ref[rows, :] = jnp.where(offset <= 0, -1.0, jnp.where(offset == 1, 0.0, backward))
        return carry

    lax.fori_loop(0, forward_ref.shape[0] // CHUNK, fill, 0, unroll=3)


def fill_starts(pair, trunc, geometry_ref, start_ref):
    rows = geometry_ref.shape[0]
    scales = []
    for order in (pair, trunc - pair):
        m = order.astype(jnp.float32)
        w = m + 8.75
        inverse = 1.0 / (w * w)
        ratio = jnp.sqrt(w) * (1.0 + inverse * (1.0 / 64.0 - (19.0 / 8192.0) * inverse))
        above = below = 1.0
        for k in range(1, 9):
            above = above * ((m + k) * (1.0 / 128.0))
            below = below * ((m + (k + 0.5)) * (1.0 / 128.0))
        scales.append((m, jnp.sqrt(ratio * above / (below * math.gamma(1.5)))))
    for first in range(0, rows, 8):
        row = lax.broadcasted_iota(jnp.int32, (8, LANES), 0) + first
        place = (2 * row + 1 - 2 * rows).astype(jnp.float32)
        _, sine = cos_sin(place, 4.0 * GRID_LATS, 0.25 / GRID_LATS)
        geometry_ref[first : first + 8, :] = -sine
        y = sine * sine
        series = jnp.full_like(y, 1.0 / 9.0)
        for k in range(8, 0, -1):
            series = series * y + 1.0 / k
        log_sine = -0.5 * y * series
        for k, (m, scale) in enumerate(scales):
            start_ref[k, first : first + 8, :] = scale * jnp.exp(m * log_sine)


def delayed(source_ref, start, delay, direction):
    options = [source_ref[pl.ds(start + direction * k, CHUNK), :] for k in range(CHUNK)]
    bit = 1
    while len(options) > 1:
        chosen = jnp.bitwise_and(delay, bit) != 0
        options = [jnp.where(chosen, options[k + 1], options[k]) for k in range(0, len(options), 2)]
        bit *= 2
    return options[0]


def legendre_step(t, latest, earlier, forward_ref, backward_ref, cosines):
    forward = forward_ref[pl.ds(t, 1), :]
    backward = backward_ref[pl.ds(t, 1), :]
    return [(forward * x) * v - backward * w for x, v, w in zip(cosines, latest, earlier)]


def first_change(trunc, pairs_total):
    least = trunc + 2 - pairs_total
    return -(-least // CHUNK)


def synthesis_kernel(
    spectrum_ref, pairs_ref, out_ref, table_ref, block_ref, raw_ref, moved_ref, kept_ref, sent_ref, forward_ref,
    backward_ref, start_ref, geometry_ref, wide_ref,
):
    share, parts, slots = spectrum_ref.shape[1:]
    trunc = slots - 2
    combos = out_ref.shape[1]
    half = out_ref.shape[0] // 2
    steps = forward_ref.shape[0]
    chunks = steps // CHUNK
    head = first_change(trunc, pairs_ref.shape[1])
    pair, delay, change = lane_facts(pairs_ref, wide_ref, share, trunc)
    fill_coefficients(pair, delay, change, trunc, forward_ref, backward_ref)
    fill_starts(pair, trunc, geometry_ref, start_ref)
    block_ref[...] = jnp.zeros_like(block_ref)
    for j in range(combos):
        source = raw_ref.at[j]
        source[:CHUNK, :] = jnp.zeros((CHUNK, LANES), jnp.float32)
        for k in range(0, slots, LANES):
            width = min(LANES, slots - k)
            tile = block_ref.at[j, k // LANES]
            tile[:share, :width] = spectrum_ref[j // parts, :, j % parts, k : k + width]
            source[pl.ds(CHUNK + k, LANES), :] = tile[...].T

        def move(chunk, carry):
            start = pl.multiple_of(chunk * CHUNK, CHUNK)
            moved_ref[j, pl.ds(start, CHUNK), :] = delayed(source, start + CHUNK, delay, -1)
            return carry

        lax.fori_loop(0, chunks, move, 0, unroll=3)
    sign = jnp.where(delay % 2 == 0, 1.0, -1.0)

    def one_group(step, carry):
        del carry
        index = [step * GROUP + k for k in range(GROUP)]
        rows = [pl.ds(pl.multiple_of(g * 8, 8), 8) for g in index]
        cosines = [geometry_ref[r, :] for r in rows]
        lows = [start_ref[0, r, :] for r in rows]
        blank = [jnp.zeros((8, LANES), jnp.float32)] * (combos * GROUP)

        def chunk_steps(start, latest, earlier, even, odd):
            even, odd = list(even), list(odd)
            for u in range(CHUNK):
                value = legendre_step(start + u, latest, earlier, forward_ref, backward_ref, cosines)
                earlier, latest = latest, value
                for g in range(GROUP):
                    kept_ref[step, start + u, g] = value[g]
                sums = even if u % 2 == 0 else odd
                for j in range(combos):
                    weight = moved_ref[j, pl.ds(start + u, 1), :]
                    for g in range(GROUP):
                        sums[j * GROUP + g] = sums[j * GROUP + g] + weight * value[g]
            return latest, earlier, even, odd

        def head_chunk(chunk, state):
            return chunk_steps(pl.multiple_of(chunk * CHUNK, CHUNK), *state)

        def tail_chunk(chunk, state):
            latest, earlier, even, odd, even_low, odd_low = state
            start = pl.multiple_of(chunk * CHUNK, CHUNK)
            now = change == start
            even_low = [jnp.where(now, a, b) for a, b in zip(even, even_low)]
            odd_low = [jnp.where(now, a, b) for a, b in zip(odd, odd_low)]
            earlier = [jnp.where(now, start_ref[1, r, :], v) for r, v in zip(rows, earlier)]
            return (*chunk_steps(start, latest, earlier, even, odd), even_low, odd_low)

        state = lax.fori_loop(0, head, head_chunk, (lows, lows, blank, blank))
        state = lax.fori_loop(head, chunks, tail_chunk, (*state, blank, blank))
        _, _, even, odd, even_low, odd_low = state
        for j in range(combos):
            for g in range(GROUP):
                k = j * GROUP + g
                mirror = 2 * half - 1 - index[g]
                out_ref[index[g], j, 0] = even_low[k] + odd_low[k]
                out_ref[mirror, j, 0] = sign * (even_low[k] - odd_low[k])
                even_high = even[k] - even_low[k]
                odd_high = odd[k] - odd_low[k]
                out_ref[index[g], j, 1] = even_high + odd_high
                out_ref[mirror, j, 1] = even_high - odd_high
        copy(step).start()
        return 0

    def copy(step):
        return pltpu.make_async_copy(kept_ref.at[step], table_ref.at[step], sent_ref.at[step])

    lax.fori_loop(0, half // GROUP, one_group, 0)
    for step in range(half // GROUP):
        copy(step).wait()


def sum_sublanes(values):
    row = lax.broadcasted_iota(jnp.int32, (8, LANES), 0)
    near = row < 4
    level = [
        jnp.where(near, values[s], values[s + 4])
        + pltpu.roll(jnp.where(near, values[s + 4], values[s]), 4, 0)
        for s in range(4)
    ]
    for width in (2, 1):
        near = jnp.bitwise_and(row, width) == 0
        level = [
            jnp.where(
                near,
                level[s] + pltpu.roll(level[s], 8 - width, 0),
                level[s + width] + pltpu.roll(level[s + width], width, 0),
            )
            for s in range(width)
        ]
    return level[0]


def truncation_kernel(
    grad_ref, pairs_ref, table_ref, out_ref, block_ref, kept_ref, come_ref, field_ref, turned_ref, final_ref, wide_ref,
):
    share, parts, slots = out_ref.shape[1:]
    combos = grad_ref.shape[1]
    half = grad_ref.shape[0] // 2
    steps = kept_ref.shape[1]
    blocks = come_ref.shape[0]
    span = steps // blocks

    def copy(k):
        rows = pl.ds(k * span, span)
        return pltpu.make_async_copy(table_ref.at[:, rows], kept_ref.at[:, rows], come_ref.at[k])

    for k in range(blocks):
        copy(k).start()
    _, delay, change = lane_facts(pairs_ref, wide_ref, share, slots - 2)
    sign = jnp.where(delay % 2 == 0, 1.0, -1.0)

    def fold(g, carry):
        for j in range(combos):
            for c in range(2):
                here = grad_ref[g, j, c]
                there = grad_ref[2 * half - 1 - g, j, c]
                if c == 0:
                    there = sign * there
                field_ref[0, c, j, g] = here + there
                field_ref[1, c, j, g] = here - there
        return carry

    lax.fori_loop(0, half, fold, 0)

    def block_steps(k, carry):
        copy(k).wait()

        def chunk_steps(chunk, carry):
            start = pl.multiple_of(k * span + chunk * CHUNK, CHUNK)
            upper = change <= start
            sums = {}
            for parity in range(2):
                for j in range(combos):
                    fields = [
                        jnp.where(upper, field_ref[parity, 1, j, g], field_ref[parity, 0, j, g]) for g in range(half)
                    ]
                    for u in range(parity, CHUNK, 2):
                        terms = [fields[g] * kept_ref[g // GROUP, start + u, g % GROUP] for g in range(half)]
                        while len(terms) > 1:
                            terms = [x + y for x, y in zip(terms[::2], terms[1::2])] + terms[len(terms) & ~1 :]
                        sums[u, j] = terms[0]
            for j in range(combos):
                turned_ref[j, pl.ds(start, CHUNK), :] = sum_sublanes([sums[u, j] for u in range(CHUNK)])
            return carry

        return lax.fori_loop(0, span // CHUNK, chunk_steps, carry)

    lax.fori_loop(0, blocks, block_steps, 0)

    for j in range(combos):
        source = turned_ref.at[j]

        def move(chunk, carry):
            start = pl.multiple_of(chunk * CHUNK, CHUNK)
            final_ref[pl.ds(start, CHUNK), :] = delayed(source, start, delay, 1)
            return carry

        lax.fori_loop(0, steps // CHUNK, move, 0, unroll=3)
        for k in range(0, slots, LANES):
            width = min(LANES, slots - k)
            tile = block_ref.at[j, k // LANES]
            tile[...] = final_ref[pl.ds(k, LANES), :].T
            out_ref[j // parts, :, j % parts, k : k + width] = tile[:share, :width]


def step_count(slots):
    return (slots + 2 * (CHUNK - 1)) // CHUNK * CHUNK


def legendre_call(kernel, name, arrays, places, out_places, out_shapes, scratch):
    space = {"v": pltpu.VMEM, "h": pltpu.HBM}
    return pl.pallas_call(
        kernel,
        in_specs=[pl.BlockSpec(memory_space=space[p]) for p in places],
        out_specs=[pl.BlockSpec(memory_space=space[p]) for p in out_places],
        out_shape=[jax.ShapeDtypeStruct(shape, jnp.float32) for shape in out_shapes],
        scratch_shapes=scratch,
        compiler_params=pltpu.CompilerParams(vmem_limit_bytes=VMEM_LIMIT),
        cost_estimate=pl.CostEstimate(flops=10**10, bytes_accessed=10**6, transcendentals=0),
        name=name,
    )(*arrays)


def f32_scratch(*shape):
    return pltpu.VMEM(shape + (LANES,), jnp.float32)


def synthesis(spectrum, pairs, window_rows):
    fields, _, parts, slots = spectrum.shape
    combos = fields * parts
    steps = step_count(slots)
    tiles = -(-slots // LANES)
    passes = window_rows // 2 // 8 // GROUP
    table = (passes, steps, GROUP, 8, LANES)
    scratch = [
        f32_scratch(combos, tiles, LANES),
        f32_scratch(combos, CHUNK + tiles * LANES),
        f32_scratch(combos, steps),
        pltpu.VMEM(table, jnp.float32),
        pltpu.SemaphoreType.DMA((passes,)),
        f32_scratch(steps),
        f32_scratch(steps),
        f32_scratch(2, window_rows // 2),
        f32_scratch(window_rows // 2),
        pair_scratch(pairs),
    ]
    shapes = [(window_rows // 8, combos, 2, 8, LANES), table]
    return legendre_call(synthesis_kernel, "synthesis", (spectrum, pairs), "vv", "vh", shapes, scratch)


def truncation(grad, pairs, table, shape):
    slots = shape[3]
    lat, combos = grad.shape[:2]
    steps = table.shape[1]
    tiles = -(-slots // LANES)
    chunks = steps // CHUNK
    blocks = next(n for n in range(min(chunks, 20), 0, -1) if chunks % n == 0)
    scratch = [
        f32_scratch(combos, tiles, LANES),
        pltpu.VMEM(table.shape, jnp.float32),
        pltpu.SemaphoreType.DMA((blocks,)),
        f32_scratch(2, 2, combos, lat // 2, 8),
        f32_scratch(combos, steps + CHUNK),
        f32_scratch(tiles * LANES),
        pair_scratch(pairs),
    ]
    return legendre_call(truncation_kernel, "truncation", (grad, pairs, table), "vvh", "v", [shape], scratch)[0]


def wave_rows(pairs_ref, wide_ref, kinds, share, trunc):
    pair = [lane_pairs(pairs_ref, wide_ref, kind, share) for kind in kinds]
    pair = jnp.concatenate(pair, axis=1) if len(pair) > 1 else pair[0]
    is_even = pair % 2 == 0
    even = jnp.where(is_even, pair, trunc - pair)
    return is_even, even.astype(jnp.float32), (trunc - even).astype(jnp.float32)


def row_place(row):
    flip = lax.axis_index("lat") >= lax.axis_size("lat") // 2
    return jnp.where(flip, 7 - row, row)


def row_tables(even, odd, length, inverse, table_refs):
    lanes = even.shape[1]
    steps = lax.broadcasted_iota(jnp.int32, (SUB, lanes), 0).astype(jnp.float32)
    for number, high_ref, low_ref in ((even, *table_refs[:2]), (odd, *table_refs[2:])):
        near_cos, near_sin = cos_sin(steps * number, length, inverse)
        far_cos, far_sin = cos_sin(steps * (number * SUB), length, inverse)
        for a in range(BLOCK // SUB):
            turn_cos = far_cos[a : a + 1, :]
            turn_sin = far_sin[a : a + 1, :]
            rows = pl.ds(a * SUB, SUB)
            high, low = split(near_cos * turn_cos - near_sin * turn_sin)
            high_ref[rows, :lanes] = high
            low_ref[rows, :lanes] = low
            high, low = split(near_sin * turn_cos + near_cos * turn_sin)
            high_ref[rows, lanes:] = high
            low_ref[rows, lanes:] = low


def outer_turns(number, blocks, length, inverse):
    steps = lax.broadcasted_iota(jnp.int32, (SUB * -(-blocks // SUB), number.shape[1]), 0).astype(jnp.float32)
    return cos_sin(steps * (number * BLOCK), length, inverse)


def three_pass(left_high, left_low, right_high, right_low, dims):
    dot = lambda a, b: lax.dot_general(a, b, (dims, ((), ())), preferred_element_type=jnp.float32)
    return dot(left_high, right_high) + (dot(left_low, right_high) + dot(left_high, right_low))


def row_kernel(kinds, share, trunc, length_ref, *refs):
    parts = len(kinds)
    part_refs = refs[:parts]
    pairs_ref, out_ref = refs[parts : parts + 2]
    table_refs = refs[parts + 2 : parts + 6]
    left_refs = refs[parts + 6 : parts + 10]
    shift_ref, wide_ref, pair_ref = refs[parts + 10 :]
    fields, nlon = out_ref.shape[1:]
    blocks = nlon // 2 // BLOCK
    row = pl.program_id(0)
    source = row_place(row)
    size = length_ref[row]
    half = size // 2
    length = size.astype(jnp.float32)
    inverse = 1.0 / jnp.full((1, LANES), length)[:, :1]
    is_even, even, odd = wave_rows(pairs_ref, pair_ref, kinds, share, trunc)
    row_tables(even, odd, length, inverse, table_refs)

    def coefficients(r, c):
        pieces = []
        for kind, ref in zip(kinds, part_refs):
            first = (r * 2 + c) * 8 + source
            if kind == "own":
                first = first + lax.axis_index("wave") * (fields * 32)
            pieces.append(ref[pl.ds(first, fields, stride=32), :])
        return jnp.concatenate(pieces, axis=1) if len(pieces) > 1 else pieces[0]

    lanes = even.shape[1]
    member = [[coefficients(r, c) for c in range(2)] for r in range(2)]
    for parity, number in ((0, even), (1, odd)):
        high_ref, low_ref = left_refs[2 * parity : 2 * parity + 2]
        weight = jnp.where(number == 0.0, 1.0, 2.0)
        real, imag = [
            jnp.where(is_even, member[r][parity], member[r][1 - parity]) * weight for r in range(2)
        ]
        turn_cos, turn_sin = outer_turns(number, blocks, length, inverse)
        for b in range(blocks):
            c = turn_cos[b : b + 1, :]
            s = turn_sin[b : b + 1, :]
            rows = pl.ds(b * fields, fields)
            high, low = split(real * c - imag * s)
            high_ref[rows, :lanes] = high
            low_ref[rows, :lanes] = low
            high, low = split(-(real * s + imag * c))
            high_ref[rows, lanes:] = high
            low_ref[rows, lanes:] = low

    dims = ((1,), (1,))
    even_sum = three_pass(left_refs[0][...], left_refs[1][...], table_refs[0][...], table_refs[1][...], dims)
    odd_sum = three_pass(left_refs[2][...], left_refs[3][...], table_refs[2][...], table_refs[3][...], dims)
    first = even_sum + odd_sum
    second = even_sum - odd_sum
    point = lax.broadcasted_iota(jnp.int32, (fields, BLOCK), 1)
    wide_ref[:, blocks * BLOCK :] = jnp.zeros((fields, wide_ref.shape[1] - blocks * BLOCK), jnp.float32)
    shift_ref[:, blocks * BLOCK :] = jnp.zeros((fields, LANES), jnp.float32)
    for b in range(blocks):
        inside = point < half - b * BLOCK
        cols = pl.ds(b * BLOCK, BLOCK)
        wide_ref[:, cols] = jnp.where(inside, first[b * fields : (b + 1) * fields], 0.0)
        shift_ref[:, cols] = jnp.where(inside, second[b * fields : (b + 1) * fields], 0.0)
    moved = pltpu.roll(shift_ref[...], half % LANES, 1)
    window = pl.ds(pl.multiple_of(half // LANES * LANES, LANES), blocks * BLOCK + LANES)
    wide_ref[:, window] = wide_ref[:, window] + moved
    out_ref[0] = wide_ref[:, :nlon]


def adjoint_kernel(kinds, share, trunc, length_ref, grad_ref, pairs_ref, *refs):
    parts = len(kinds)
    part_refs = refs[:parts]
    table_refs = refs[parts : parts + 4]
    left_refs = refs[parts + 4 : parts + 8]
    wide_ref, pair_ref = refs[parts + 8 :]
    fields, nlon = grad_ref.shape[1:]
    blocks = nlon // 2 // BLOCK
    row = pl.program_id(0)
    target = row_place(row)
    size = length_ref[row]
    half = size // 2
    length = size.astype(jnp.float32)
    inverse = 1.0 / jnp.full((1, LANES), length)[:, :1]
    is_even, even, odd = wave_rows(pairs_ref, pair_ref, kinds, share, trunc)
    row_tables(even, odd, length, inverse, table_refs)
    wide_ref[:, :nlon] = grad_ref[0]
    wide_ref[:, nlon:] = jnp.zeros((fields, wide_ref.shape[1] - nlon), jnp.float32)
    span = blocks * BLOCK + LANES
    window = pl.ds(pl.multiple_of(half // LANES * LANES, LANES), span)
    moved = pltpu.roll(wide_ref[:, window], (span - half % LANES) % span, 1)
    point = lax.broadcasted_iota(jnp.int32, (fields, BLOCK), 1)
    for b in range(blocks):
        inside = point < half - b * BLOCK
        cols = slice(b * BLOCK, (b + 1) * BLOCK)
        rows = pl.ds(b * fields, fields)
        first = jnp.where(inside, grad_ref[0, :, cols], 0.0)
        second = jnp.where(inside, moved[:, cols], 0.0)
        left_refs[0][rows, :], left_refs[1][rows, :] = split(first + second)
        left_refs[2][rows, :], left_refs[3][rows, :] = split(first - second)
    dims = ((1,), (0,))
    lanes = even.shape[1]
    result = []
    for parity, number in ((0, even), (1, odd)):
        k = 2 * parity
        folded = three_pass(
            left_refs[k][...], left_refs[k + 1][...], table_refs[k][...], table_refs[k + 1][...], dims
        )
        turn_cos, turn_sin = outer_turns(number, blocks, length, inverse)
        real = imag = 0.0
        for b in range(blocks):
            c = turn_cos[b : b + 1, :]
            s = turn_sin[b : b + 1, :]
            cos_part = folded[b * fields : (b + 1) * fields, :lanes]
            sin_part = folded[b * fields : (b + 1) * fields, lanes:]
            real = real + (c * cos_part - s * sin_part)
            imag = imag - (s * cos_part + c * sin_part)
        weight = jnp.where(number == 0.0, 1.0, 2.0)
        result.append((weight * real, weight * imag))
    for r in range(2):
        for c in range(2):
            value = jnp.where(is_even, result[c][r], result[1 - c][r])
            start = 0
            for kind, ref in zip(kinds, part_refs):
                first = (r * 2 + c) * 8 + target
                if kind == "own":
                    first = first + lax.axis_index("wave") * (fields * 32)
                ref[pl.ds(first, fields, stride=32), :] = value[:, start : start + LANES]
                start += LANES


def row_scratch(blocks, fields, lanes, nlon, left_width):
    bf16 = jnp.bfloat16
    tables = [pltpu.VMEM((BLOCK, 2 * lanes), bf16)] * 4
    lefts = [pltpu.VMEM((blocks * fields, left_width), bf16)] * 4
    return tables, lefts


def whole_block(shape):
    return pl.BlockSpec(shape, lambda i, *_: (0,) * len(shape))


def pair_scratch(pairs):
    return pltpu.VMEM((8, -(-pairs.shape[1] // LANES) * LANES), jnp.int32)


def rows_out(parts, kinds, share, pairs, row_length, fields, nlon, trunc):
    row_dev = row_length.shape[0]
    lanes = LANES * len(kinds)
    blocks = nlon // 2 // BLOCK
    tables, lefts = row_scratch(blocks, fields, lanes, nlon, 2 * lanes)
    parts = [p.reshape(-1, LANES) for p in parts]
    span = blocks * BLOCK + LANES
    return pl.pallas_call(
        lambda *refs: row_kernel(kinds, share, trunc, *refs),
        grid_spec=pltpu.PrefetchScalarGridSpec(
            num_scalar_prefetch=1,
            grid=(row_dev,),
            in_specs=[whole_block(p.shape) for p in parts] + [whole_block(pairs.shape)],
            out_specs=pl.BlockSpec((1, fields, nlon), lambda i, *_: (i, 0, 0)),
            scratch_shapes=tables
            + lefts
            + [
                pltpu.VMEM((fields, span), jnp.float32),
                pltpu.VMEM((fields, nlon // 2 + span), jnp.float32),
                pair_scratch(pairs),
            ],
        ),
        out_shape=jax.ShapeDtypeStruct((row_dev, fields, nlon), jnp.float32),
        compiler_params=pltpu.CompilerParams(vmem_limit_bytes=VMEM_LIMIT),
        cost_estimate=pl.CostEstimate(flops=10**10, bytes_accessed=10**6, transcendentals=0),
        name="rows",
    )(row_length, *parts, pairs)


def rows_adjoint(grad_grid, kinds, share, heights, pairs, row_length, trunc):
    row_dev, fields, nlon = grad_grid.shape
    lanes = LANES * len(kinds)
    blocks = nlon // 2 // BLOCK
    tables, lefts = row_scratch(blocks, fields, lanes, nlon, BLOCK)
    shapes = [(height * 32, LANES) for height in heights]
    span = blocks * BLOCK + LANES
    return pl.pallas_call(
        lambda *refs: adjoint_kernel(kinds, share, trunc, *refs),
        grid_spec=pltpu.PrefetchScalarGridSpec(
            num_scalar_prefetch=1,
            grid=(row_dev,),
            in_specs=[pl.BlockSpec((1, fields, nlon), lambda i, *_: (i, 0, 0)), whole_block(pairs.shape)],
            out_specs=[whole_block(s) for s in shapes],
            scratch_shapes=tables
            + lefts
            + [pltpu.VMEM((fields, nlon // 2 + span), jnp.float32), pair_scratch(pairs)],
        ),
        out_shape=[jax.ShapeDtypeStruct(s, jnp.float32) for s in shapes],
        compiler_params=pltpu.CompilerParams(vmem_limit_bytes=VMEM_LIMIT),
        cost_estimate=pl.CostEstimate(flops=10**10, bytes_accessed=10**6, transcendentals=0),
        name="adjoint",
    )(row_length, grad_grid, pairs)


def body(spectrum, grad_grid, row_length, pair_of_slot):
    row_dev, grid_fields, nlon = grad_grid.shape
    own_fields, share, _, slots = spectrum.shape
    trunc = slots - 2
    lat = lax.axis_size("lat")
    wave = lax.axis_size("wave")
    wave_index = lax.axis_index("wave")
    combos = own_fields * 2
    total = pair_of_slot.shape[0]
    pairs = pair_of_slot[None, :]
    two = wave == 2
    swap = [(0, 1), (1, 0)]
    tiles = tuple(range(-(-total // LANES)))
    shape = (lat, combos, 2, 8, LANES)

    coeffs, table = synthesis(spectrum, pairs, row_dev * lat)
    coeffs = lax.all_to_all(coeffs, "lat", split_axis=0, concat_axis=0, tiled=True)

    if two:
        kinds = ("own", "other")
        heights = (2 * grid_fields, grid_fields)
        kept, sent = rows_adjoint(grad_grid, kinds, share, heights, pairs, row_length, trunc)
        received = lax.ppermute(sent, "wave", swap)
        start = (1 - wave_index) * received.shape[0]
        grads = lax.dynamic_update_slice_in_dim(kept, received, start, 0).reshape(shape)
    else:
        folded = rows_adjoint(grad_grid, tiles, share, (grid_fields,) * len(tiles), pairs, row_length, trunc)
        turned = jnp.concatenate(folded, axis=1)[:, :total].reshape(-1, wave, share)
        turned = jnp.pad(jnp.transpose(turned, (1, 0, 2)), ((0, 0), (0, 0), (0, LANES - share)))
        grads = lax.all_to_all(turned, "wave", split_axis=0, concat_axis=0, tiled=True).reshape(shape)
    grads = lax.all_to_all(grads, "lat", split_axis=0, concat_axis=0, tiled=True)

    if two:
        outgoing = lax.dynamic_slice_in_dim(coeffs, (1 - wave_index) * (lat // 2), lat // 2)
        parts = [coeffs, lax.ppermute(outgoing, "wave", swap)]
    else:
        turned = lax.all_to_all(coeffs, "wave", split_axis=0, concat_axis=0, tiled=True)
        turned = turned.reshape(wave, -1, LANES)[:, :, :share]
        turned = jnp.transpose(turned, (1, 0, 2)).reshape(turned.shape[1], -1)
        turned = jnp.pad(turned, ((0, 0), (0, LANES * len(tiles) - total)))
        parts = [turned[:, k * LANES : (k + 1) * LANES] for k in tiles]
        kinds = tiles
    grid_field = rows_out(parts, kinds, share, pairs, row_length, grid_fields, nlon, trunc)

    grads, grid_field = lax.optimization_barrier((grads, grid_field))
    return grid_field, truncation(grads, pairs, table, spectrum.shape)


def solution(mesh):
    placed = (P("lat", "wave", None, None), P("lat", "wave", None), P("lat"), P())
    return jax.shard_map(
        body,
        mesh=mesh,
        in_specs=placed,
        out_specs=(P("lat", "wave", None), P("lat", "wave", None, None)),
        check_vma=False,
    )
```

```python
import math

import jax
import jax.numpy as jnp
import numpy as np
from jax import lax
from jax.experimental import pallas as pl
from jax.experimental.pallas import tpu as pltpu
from jax.sharding import PartitionSpec as P

GRID_LATS = 2560
LANES = 128
BLOCK = 256
SUB = 16
CHUNK = 8
GROUP = 2
AHEAD = 9
SYNTHESIS_VMEM = 56 * 1024 * 1024
TRUNCATION_VMEM = 52 * 1024 * 1024
ROW_VMEM = 20 * 1024 * 1024


def fit_trig():
    nodes = np.cos(np.pi * (np.arange(400) + 0.5) / 400)
    y = 0.125 * (nodes + 1.0) * 1.01
    u = np.sqrt(y)
    sin_fit = np.polynomial.chebyshev.Chebyshev.fit(y, np.sin(2 * np.pi * u) / u, 7, domain=[0, 0.2525])
    cos_fit = np.polynomial.chebyshev.Chebyshev.fit(y, np.cos(2 * np.pi * u), 8, domain=[0, 0.2525])
    to_power = lambda fit: [float(c) for c in fit.convert(kind=np.polynomial.Polynomial).coef]
    return to_power(sin_fit), to_power(cos_fit)


SIN_COEF, COS_COEF = fit_trig()


def horner(coefs, y):
    value = jnp.full_like(y, coefs[-1])
    for c in coefs[-2::-1]:
        value = value * y + c
    return value


def cos_sin(product, length, inverse):
    turns = jnp.floor(product * inverse + 0.5)
    u = (product - turns * length) * inverse
    y = u * u
    return horner(COS_COEF, y), u * horner(SIN_COEF, y)


def split(value):
    high = value.astype(jnp.bfloat16)
    low = (value - high.astype(jnp.float32)).astype(jnp.bfloat16)
    return high, low


def lane_pairs(pairs_ref, wide_ref, kind, share):
    total = pairs_ref.shape[1]
    width = wide_ref.shape[1]
    if kind in ("own", "other"):
        wave = lax.axis_index("wave")
        first = share * (wave if kind == "own" else 1 - wave)
        valid = share
    else:
        first = LANES * kind
        valid = min(LANES, total - first)
    wide_ref[0:1, :total] = pairs_ref[...]
    lanes = pltpu.roll(wide_ref[...], (width - first) % width, 1)[0:1, :LANES]
    return jnp.where(lax.broadcasted_iota(jnp.int32, (1, LANES), 1) < valid, lanes, 0)


def lane_facts(pairs_ref, wide_ref, share, trunc):
    pair = lane_pairs(pairs_ref, wide_ref, "own", share)
    boundary = trunc + 1 - pair
    delay = jnp.bitwise_and(-boundary, CHUNK - 1)
    return pair, delay, boundary + delay


def fill_coefficients(pair, delay, change, trunc, forward_ref, backward_ref):
    low_order = pair.astype(jnp.float32)
    high_order = trunc - low_order

    def fill(chunk, carry):
        step = lax.broadcasted_iota(jnp.int32, (CHUNK, LANES), 0) + chunk * CHUNK
        upper = step >= change
        order = jnp.where(upper, high_order, low_order)
        offset = jnp.where(upper, step - change, step - delay)
        degree = order + offset.astype(jnp.float32)
        lower = degree - 1.0
        top = jnp.maximum(4.0 * degree * degree - 1.0, 1.0)
        base = jnp.maximum(degree * degree - order * order, 1.0)
        lower_top = jnp.maximum(4.0 * lower * lower - 1.0, 1.0)
        lower_base = jnp.maximum(lower * lower - order * order, 1.0)
        forward = jnp.sqrt(top / base)
        backward = jnp.sqrt((top * lower_base) / (base * lower_top))
        rows = pl.ds(pl.multiple_of(chunk * CHUNK, CHUNK), CHUNK)
        forward_ref[rows, :] = jnp.where(offset <= 0, 0.0, forward)
        backward_ref[rows, :] = jnp.where(offset <= 0, -1.0, jnp.where(offset == 1, 0.0, backward))
        return carry

    lax.fori_loop(0, forward_ref.shape[0] // CHUNK, fill, 0, unroll=3)


def fill_starts(pair, trunc, geometry_ref, start_ref):
    rows = geometry_ref.shape[0]
    scales = []
    for order in (pair, trunc - pair):
        m = order.astype(jnp.float32)
        w = m + 8.75
        inverse = 1.0 / (w * w)
        ratio = jnp.sqrt(w) * (1.0 + inverse * (1.0 / 64.0 - (19.0 / 8192.0) * inverse))
        above = below = 1.0
        for k in range(1, 9):
            above = above * ((m + k) * (1.0 / 128.0))
            below = below * ((m + (k + 0.5)) * (1.0 / 128.0))
        scales.append((m, jnp.sqrt(ratio * above / (below * math.gamma(1.5)))))
    for first in range(0, rows, 8):
        row = lax.broadcasted_iota(jnp.int32, (8, LANES), 0) + first
        place = (2 * row + 1 - 2 * rows).astype(jnp.float32)
        _, sine = cos_sin(place, 4.0 * GRID_LATS, 0.25 / GRID_LATS)
        geometry_ref[first : first + 8, :] = -sine
        y = sine * sine
        series = jnp.full_like(y, 1.0 / 9.0)
        for k in range(8, 0, -1):
            series = series * y + 1.0 / k
        log_sine = -0.5 * y * series
        for k, (m, scale) in enumerate(scales):
            start_ref[k, first : first + 8, :] = scale * jnp.exp(m * log_sine)


def delayed(source_ref, start, delay, direction):
    options = [source_ref[pl.ds(start + direction * k, CHUNK), :] for k in range(CHUNK)]
    bit = 1
    while len(options) > 1:
        chosen = jnp.bitwise_and(delay, bit) != 0
        options = [jnp.where(chosen, options[k + 1], options[k]) for k in range(0, len(options), 2)]
        bit *= 2
    return options[0]


def legendre_step(t, latest, earlier, forward_ref, backward_ref, cosines):
    forward = forward_ref[pl.ds(t, 1), :]
    backward = backward_ref[pl.ds(t, 1), :]
    return [(forward * x) * v - backward * w for x, v, w in zip(cosines, latest, earlier)]


def first_change(trunc, pairs_total):
    least = trunc + 2 - pairs_total
    return -(-least // CHUNK)


def synthesis_kernel(
    remote_ref, pairs_ref, out_ref, table_ref, spectrum_ref, near_ref, block_ref, raw_ref, moved_ref, kept_ref, sent_ref, forward_ref,
    backward_ref, start_ref, geometry_ref, wide_ref,
):
    local = pltpu.make_async_copy(remote_ref, spectrum_ref, near_ref)
    local.start()
    share, parts, slots = spectrum_ref.shape[1:]
    trunc = slots - 2
    combos = out_ref.shape[1]
    half = out_ref.shape[0] // 2
    steps = forward_ref.shape[0]
    chunks = steps // CHUNK
    head = first_change(trunc, pairs_ref.shape[1])
    pair, delay, change = lane_facts(pairs_ref, wide_ref, share, trunc)
    fill_coefficients(pair, delay, change, trunc, forward_ref, backward_ref)
    fill_starts(pair, trunc, geometry_ref, start_ref)
    block_ref[...] = jnp.zeros_like(block_ref)
    local.wait()
    for j in range(combos):
        source = raw_ref.at[j]
        source[:CHUNK, :] = jnp.zeros((CHUNK, LANES), jnp.float32)
        for k in range(0, slots, LANES):
            width = min(LANES, slots - k)
            tile = block_ref.at[j, k // LANES]
            tile[:share, :width] = spectrum_ref[j // parts, :, j % parts, k : k + width]
            source[pl.ds(CHUNK + k, LANES), :] = tile[...].T

        def move(chunk, carry):
            start = pl.multiple_of(chunk * CHUNK, CHUNK)
            moved_ref[j, pl.ds(start, CHUNK), :] = delayed(source, start + CHUNK, delay, -1)
            return carry

        lax.fori_loop(0, chunks, move, 0, unroll=3)
    sign = jnp.where(delay % 2 == 0, 1.0, -1.0)

    def one_group(step, carry):
        del carry
        index = [step * GROUP + k for k in range(GROUP)]
        rows = [pl.ds(pl.multiple_of(g * 8, 8), 8) for g in index]
        cosines = [geometry_ref[r, :] for r in rows]
        lows = [start_ref[0, r, :] for r in rows]
        blank = [jnp.zeros((8, LANES), jnp.float32)] * (combos * GROUP)

        def chunk_steps(start, latest, earlier, even, odd):
            even, odd = list(even), list(odd)
            for u in range(CHUNK):
                value = legendre_step(start + u, latest, earlier, forward_ref, backward_ref, cosines)
                earlier, latest = latest, value
                for g in range(GROUP):
                    kept_ref[step, start + u, g] = value[g]
                sums = even if u % 2 == 0 else odd
                for j in range(combos):
                    weight = moved_ref[j, pl.ds(start + u, 1), :]
                    for g in range(GROUP):
                        sums[j * GROUP + g] = sums[j * GROUP + g] + weight * value[g]
            return latest, earlier, even, odd

        def head_chunk(chunk, state):
            return chunk_steps(pl.multiple_of(chunk * CHUNK, CHUNK), *state)

        def tail_chunk(chunk, state):
            latest, earlier, even, odd, even_low, odd_low = state
            start = pl.multiple_of(chunk * CHUNK, CHUNK)
            now = change == start
            even_low = [jnp.where(now, a, b) for a, b in zip(even, even_low)]
            odd_low = [jnp.where(now, a, b) for a, b in zip(odd, odd_low)]
            earlier = [jnp.where(now, start_ref[1, r, :], v) for r, v in zip(rows, earlier)]
            return (*chunk_steps(start, latest, earlier, even, odd), even_low, odd_low)

        state = lax.fori_loop(0, head, head_chunk, (lows, lows, blank, blank))
        copy(step, 0).start()
        state = lax.fori_loop(head, chunks, tail_chunk, (*state, blank, blank))
        _, _, even, odd, even_low, odd_low = state
        for j in range(combos):
            for g in range(GROUP):
                k = j * GROUP + g
                mirror = 2 * half - 1 - index[g]
                out_ref[index[g], j, 0] = even_low[k] + odd_low[k]
                out_ref[mirror, j, 0] = sign * (even_low[k] - odd_low[k])
                even_high = even[k] - even_low[k]
                odd_high = odd[k] - odd_low[k]
                out_ref[index[g], j, 1] = even_high + odd_high
                out_ref[mirror, j, 1] = even_high - odd_high
        copy(step, 1).start()
        return 0

    def copy(step, piece):
        rows = pl.ds(head * CHUNK, steps - head * CHUNK) if piece else pl.ds(0, head * CHUNK)
        return pltpu.make_async_copy(kept_ref.at[step, rows], table_ref.at[step, rows], sent_ref.at[step, piece])

    lax.fori_loop(0, half // GROUP, one_group, 0)
    for step in range(half // GROUP):
        copy(step, 0).wait()
        copy(step, 1).wait()


def sum_sublanes(values):
    row = lax.broadcasted_iota(jnp.int32, (8, LANES), 0)
    near = row < 4
    level = [
        jnp.where(near, values[s], values[s + 4])
        + pltpu.roll(jnp.where(near, values[s + 4], values[s]), 4, 0)
        for s in range(4)
    ]
    for width in (2, 1):
        near = jnp.bitwise_and(row, width) == 0
        level = [
            jnp.where(
                near,
                level[s] + pltpu.roll(level[s], 8 - width, 0),
                level[s + width] + pltpu.roll(level[s + width], width, 0),
            )
            for s in range(width)
        ]
    return level[0]


def truncation_kernel(
    grad_ref, pairs_ref, table_ref, out_ref, block_ref, kept_ref, come_ref, field_ref, turned_ref, final_ref, wide_ref,
):
    share, parts, slots = out_ref.shape[1:]
    combos = grad_ref.shape[1] // 2
    half = grad_ref.shape[0] // 2
    steps = kept_ref.shape[1]
    blocks = come_ref.shape[0]
    span = steps // blocks

    def copy(k):
        rows = pl.ds(k * span, span)
        return pltpu.make_async_copy(table_ref.at[:, rows], kept_ref.at[:, rows], come_ref.at[k])

    for k in range(min(AHEAD, blocks)):
        copy(k).start()
    _, delay, change = lane_facts(pairs_ref, wide_ref, share, slots - 2)
    sign = jnp.where(delay % 2 == 0, 1.0, -1.0)

    def fold(g, carry):
        for j in range(combos):
            for c in range(2):
                here = grad_ref[g, 2 * j + c]
                there = grad_ref[2 * half - 1 - g, 2 * j + c]
                if c == 0:
                    there = sign * there
                field_ref[0, c, j, g] = here + there
                field_ref[1, c, j, g] = here - there
        return carry

    lax.fori_loop(0, half, fold, 0)

    def block_steps(k, carry):
        copy(k).wait()

        @pl.when(k + AHEAD < blocks)
        def _():
            copy(k + AHEAD).start()

        def chunk_steps(chunk, carry):
            start = pl.multiple_of(k * span + chunk * CHUNK, CHUNK)
            upper = change <= start
            sums = {}
            for parity in range(2):
                for j in range(combos):
                    fields = [
                        jnp.where(upper, field_ref[parity, 1, j, g], field_ref[parity, 0, j, g]) for g in range(half)
                    ]
                    for u in range(parity, CHUNK, 2):
                        terms = [fields[g] * kept_ref[g // GROUP, start + u, g % GROUP] for g in range(half)]
                        while len(terms) > 1:
                            terms = [x + y for x, y in zip(terms[::2], terms[1::2])] + terms[len(terms) & ~1 :]
                        sums[u, j] = terms[0]
            for j in range(combos):
                turned_ref[j, pl.ds(start, CHUNK), :] = sum_sublanes([sums[u, j] for u in range(CHUNK)])
            return carry

        return lax.fori_loop(0, span // CHUNK, chunk_steps, carry)

    lax.fori_loop(0, blocks, block_steps, 0)

    for j in range(combos):
        source = turned_ref.at[j]

        def move(chunk, carry):
            start = pl.multiple_of(chunk * CHUNK, CHUNK)
            final_ref[pl.ds(start, CHUNK), :] = delayed(source, start, delay, 1)
            return carry

        lax.fori_loop(0, steps // CHUNK, move, 0, unroll=3)
        for k in range(0, slots, LANES):
            width = min(LANES, slots - k)
            tile = block_ref.at[j, k // LANES]
            tile[...] = final_ref[pl.ds(k, LANES), :].T
            out_ref[j // parts, :, j % parts, k : k + width] = tile[:share, :width]


def step_count(slots):
    return (slots + 2 * (CHUNK - 1)) // CHUNK * CHUNK


def legendre_call(kernel, name, arrays, places, out_places, out_shapes, scratch, limit):
    space = {"v": pltpu.VMEM, "h": pltpu.HBM}
    return pl.pallas_call(
        kernel,
        in_specs=[pl.BlockSpec(memory_space=space[p]) for p in places],
        out_specs=[pl.BlockSpec(memory_space=space[p]) for p in out_places],
        out_shape=[jax.ShapeDtypeStruct(shape, jnp.float32) for shape in out_shapes],
        scratch_shapes=scratch,
        compiler_params=pltpu.CompilerParams(vmem_limit_bytes=limit),
        cost_estimate=pl.CostEstimate(flops=10**10, bytes_accessed=10**6, transcendentals=0),
        name=name,
    )(*arrays)


def f32_scratch(*shape):
    return pltpu.VMEM(shape + (LANES,), jnp.float32)


def synthesis(spectrum, pairs, window_rows):
    fields, _, parts, slots = spectrum.shape
    combos = fields * parts
    steps = step_count(slots)
    tiles = -(-slots // LANES)
    passes = window_rows // 2 // 8 // GROUP
    table = (passes, steps, GROUP, 8, LANES)
    scratch = [
        pltpu.VMEM(spectrum.shape, jnp.float32),
        pltpu.SemaphoreType.DMA(()),
        f32_scratch(combos, tiles, LANES),
        f32_scratch(combos, CHUNK + tiles * LANES),
        f32_scratch(combos, steps),
        pltpu.VMEM(table, jnp.float32),
        pltpu.SemaphoreType.DMA((passes, 2)),
        f32_scratch(steps),
        f32_scratch(steps),
        f32_scratch(2, window_rows // 2),
        f32_scratch(window_rows // 2),
        pair_scratch(pairs),
    ]
    shapes = [(window_rows // 8, combos, 2, 8, LANES), table]
    return legendre_call(synthesis_kernel, "synthesis", (spectrum, pairs), "hv", "vh", shapes, scratch, SYNTHESIS_VMEM)


def truncation(grad, pairs, table, shape):
    slots = shape[3]
    lat, combos = grad.shape[:2]
    combos = combos // 2
    steps = table.shape[1]
    tiles = -(-slots // LANES)
    chunks = steps // CHUNK
    blocks = next(n for n in range(min(chunks, 20), 0, -1) if chunks % n == 0)
    scratch = [
        f32_scratch(combos, tiles, LANES),
        pltpu.VMEM(table.shape, jnp.float32),
        pltpu.SemaphoreType.DMA((blocks,)),
        f32_scratch(2, 2, combos, lat // 2, 8),
        f32_scratch(combos, steps + CHUNK),
        f32_scratch(tiles * LANES),
        pair_scratch(pairs),
    ]
    arrays = (grad, pairs, table)
    return legendre_call(truncation_kernel, "truncation", arrays, "vvh", "v", [shape], scratch, TRUNCATION_VMEM)[0]


def wave_rows(pairs_ref, wide_ref, kinds, share, trunc):
    pair = [lane_pairs(pairs_ref, wide_ref, kind, share) for kind in kinds]
    pair = jnp.concatenate(pair, axis=1) if len(pair) > 1 else pair[0]
    is_even = pair % 2 == 0
    even = jnp.where(is_even, pair, trunc - pair)
    return is_even, even.astype(jnp.float32), (trunc - even).astype(jnp.float32)


def row_place(row):
    flip = lax.axis_index("lat") >= lax.axis_size("lat") // 2
    return jnp.where(flip, 7 - row, row)


def row_tables(even, odd, length, inverse, table_refs):
    lanes = even.shape[1]
    steps = lax.broadcasted_iota(jnp.int32, (SUB, lanes), 0).astype(jnp.float32)
    for number, high_ref, low_ref in ((even, *table_refs[:2]), (odd, *table_refs[2:])):
        near_cos, near_sin = cos_sin(steps * number, length, inverse)
        far_cos, far_sin = cos_sin(steps * (number * SUB), length, inverse)
        for a in range(BLOCK // SUB):
            turn_cos = far_cos[a : a + 1, :]
            turn_sin = far_sin[a : a + 1, :]
            rows = pl.ds(a * SUB, SUB)
            high, low = split(near_cos * turn_cos - near_sin * turn_sin)
            high_ref[rows, :lanes] = high
            low_ref[rows, :lanes] = low
            high, low = split(near_sin * turn_cos + near_cos * turn_sin)
            high_ref[rows, lanes:] = high
            low_ref[rows, lanes:] = low


def outer_turns(number, blocks, length, inverse):
    steps = lax.broadcasted_iota(jnp.int32, (SUB * -(-blocks // SUB), number.shape[1]), 0).astype(jnp.float32)
    return cos_sin(steps * (number * BLOCK), length, inverse)


def three_pass(left_high, left_low, right_high, right_low, dims):
    dot = lambda a, b: lax.dot_general(a, b, (dims, ((), ())), preferred_element_type=jnp.float32)
    return dot(left_high, right_high) + (dot(left_low, right_high) + dot(left_high, right_low))


def row_kernel(kinds, share, trunc, length_ref, *refs):
    parts = len(kinds)
    part_refs = refs[:parts]
    pairs_ref, out_ref = refs[parts : parts + 2]
    table_refs = refs[parts + 2 : parts + 6]
    left_refs = refs[parts + 6 : parts + 10]
    shift_ref, wide_ref, pair_ref = refs[parts + 10 :]
    fields, nlon = out_ref.shape[1:]
    blocks = nlon // 2 // BLOCK
    row = pl.program_id(0)
    source = row_place(row)
    size = length_ref[row]
    half = size // 2
    length = size.astype(jnp.float32)
    inverse = 1.0 / jnp.full((1, LANES), length)[:, :1]
    is_even, even, odd = wave_rows(pairs_ref, pair_ref, kinds, share, trunc)
    row_tables(even, odd, length, inverse, table_refs)

    def coefficients(r, c):
        pieces = []
        for kind, ref in zip(kinds, part_refs):
            first = (r * 2 + c) * 8 + source
            if kind == "own":
                first = first + lax.axis_index("wave") * (fields * 32)
            pieces.append(ref[pl.ds(first, fields, stride=32), :])
        return jnp.concatenate(pieces, axis=1) if len(pieces) > 1 else pieces[0]

    lanes = even.shape[1]
    member = [[coefficients(r, c) for c in range(2)] for r in range(2)]
    for parity, number in ((0, even), (1, odd)):
        high_ref, low_ref = left_refs[2 * parity : 2 * parity + 2]
        weight = jnp.where(number == 0.0, 1.0, 2.0)
        real, imag = [
            jnp.where(is_even, member[r][parity], member[r][1 - parity]) * weight for r in range(2)
        ]
        turn_cos, turn_sin = outer_turns(number, blocks, length, inverse)
        for b in range(blocks):
            c = turn_cos[b : b + 1, :]
            s = turn_sin[b : b + 1, :]
            rows = pl.ds(b * fields, fields)
            high, low = split(real * c - imag * s)
            high_ref[rows, :lanes] = high
            low_ref[rows, :lanes] = low
            high, low = split(-(real * s + imag * c))
            high_ref[rows, lanes:] = high
            low_ref[rows, lanes:] = low

    dims = ((1,), (1,))
    even_sum = three_pass(left_refs[0][...], left_refs[1][...], table_refs[0][...], table_refs[1][...], dims)
    odd_sum = three_pass(left_refs[2][...], left_refs[3][...], table_refs[2][...], table_refs[3][...], dims)
    first = even_sum + odd_sum
    second = even_sum - odd_sum
    point = lax.broadcasted_iota(jnp.int32, (fields, BLOCK), 1)
    wide_ref[:, blocks * BLOCK :] = jnp.zeros((fields, wide_ref.shape[1] - blocks * BLOCK), jnp.float32)
    shift_ref[:, blocks * BLOCK :] = jnp.zeros((fields, LANES), jnp.float32)
    for b in range(blocks):
        inside = point < half - b * BLOCK
        cols = pl.ds(b * BLOCK, BLOCK)
        wide_ref[:, cols] = jnp.where(inside, first[b * fields : (b + 1) * fields], 0.0)
        shift_ref[:, cols] = jnp.where(inside, second[b * fields : (b + 1) * fields], 0.0)
    moved = pltpu.roll(shift_ref[...], half % LANES, 1)
    window = pl.ds(pl.multiple_of(half // LANES * LANES, LANES), blocks * BLOCK + LANES)
    wide_ref[:, window] = wide_ref[:, window] + moved
    out_ref[0] = wide_ref[:, :nlon]


def adjoint_kernel(kinds, share, trunc, grad_shape, length_ref, grad_ref, pairs_ref, *refs):
    parts = len(kinds)
    part_refs = refs[:parts]
    wide_ref, come_ref, pair_ref = refs[parts : parts + 3]
    count, fields, nlon = grad_shape
    blocks = nlon // 2 // BLOCK

    def copy(place):
        row = row_place(place)
        return pltpu.make_async_copy(grad_ref.at[row], wide_ref.at[place, :, pl.ds(0, nlon)], come_ref.at[place])

    for place in range(min(2, count)):
        copy(place).start()
    is_even, even, odd = wave_rows(pairs_ref, pair_ref, kinds, share, trunc)
    lanes = even.shape[1]
    span = blocks * BLOCK + LANES
    point = lax.broadcasted_iota(jnp.int32, (fields, BLOCK), 1)

    def one_row(place, table_refs, left_refs):
        size = length_ref[row_place(place)]
        half = size // 2
        length = size.astype(jnp.float32)
        inverse = 1.0 / jnp.full((1, LANES), length)[:, :1]
        row_tables(even, odd, length, inverse, table_refs)
        copy(place).wait()

        @pl.when(place + 2 < count)
        def _():
            copy(place + 2).start()

        window = pl.ds(pl.multiple_of(half // LANES * LANES, LANES), span)
        moved = pltpu.roll(wide_ref[place, :, window], (span - half % LANES) % span, 1)
        for b in range(blocks):
            inside = point < half - b * BLOCK
            cols = slice(b * BLOCK, (b + 1) * BLOCK)
            rows = pl.ds(b * fields, fields)
            early = jnp.where(inside, wide_ref[place, :, cols], 0.0)
            late = jnp.where(inside, moved[:, cols], 0.0)
            left_refs[0][rows, :], left_refs[1][rows, :] = split(early + late)
            left_refs[2][rows, :], left_refs[3][rows, :] = split(early - late)
        dims = ((1,), (0,))
        result = []
        for parity, number in ((0, even), (1, odd)):
            k = 2 * parity
            folded = three_pass(
                left_refs[k][...], left_refs[k + 1][...], table_refs[k][...], table_refs[k + 1][...], dims
            )
            turn_cos, turn_sin = outer_turns(number, blocks, length, inverse)
            real = imag = 0.0
            for b in range(blocks):
                c = turn_cos[b : b + 1, :]
                s = turn_sin[b : b + 1, :]
                cos_part = folded[b * fields : (b + 1) * fields, :lanes]
                sin_part = folded[b * fields : (b + 1) * fields, lanes:]
                real = real + (c * cos_part - s * sin_part)
                imag = imag - (s * cos_part + c * sin_part)
            weight = jnp.where(number == 0.0, 1.0, 2.0)
            result.append((weight * real, weight * imag))
        for r in range(2):
            for c in range(2):
                value = jnp.where(is_even, result[c][r], result[1 - c][r])
                start = 0
                for kind, ref in zip(kinds, part_refs):
                    top = (r * 2 + c) * count + place
                    if kind == "own":
                        top = top + lax.axis_index("wave") * (fields * 4 * count)
                    ref[pl.ds(top, fields, stride=4 * count), :] = value[:, start : start + LANES]
                    start += LANES

    def step(place, carry):
        one_row(place, refs[parts + 3 : parts + 7], refs[parts + 7 :])
        return carry

    lax.fori_loop(0, count, step, 0)


def row_scratch(blocks, fields, lanes, nlon, left_width):
    bf16 = jnp.bfloat16
    tables = [pltpu.VMEM((BLOCK, 2 * lanes), bf16)] * 4
    lefts = [pltpu.VMEM((blocks * fields, left_width), bf16)] * 4
    return tables, lefts


def pair_scratch(pairs):
    return pltpu.VMEM((8, -(-pairs.shape[1] // LANES) * LANES), jnp.int32)


def rows_out(parts, kinds, share, pairs, row_length, fields, nlon, trunc):
    row_dev = row_length.shape[0]
    lanes = LANES * len(kinds)
    blocks = nlon // 2 // BLOCK
    tables, lefts = row_scratch(blocks, fields, lanes, nlon, 2 * lanes)
    parts = [p.reshape(-1, LANES) for p in parts]
    span = blocks * BLOCK + LANES
    return pl.pallas_call(
        lambda *refs: row_kernel(kinds, share, trunc, *refs),
        grid_spec=pltpu.PrefetchScalarGridSpec(
            num_scalar_prefetch=1,
            grid=(row_dev,),
            in_specs=[pl.BlockSpec(memory_space=pltpu.VMEM)] * (len(parts) + 1),
            out_specs=pl.BlockSpec((1, fields, nlon), lambda i, *_: (i, 0, 0)),
            scratch_shapes=tables
            + lefts
            + [
                pltpu.VMEM((fields, span), jnp.float32),
                pltpu.VMEM((fields, nlon // 2 + span), jnp.float32),
                pair_scratch(pairs),
            ],
        ),
        out_shape=jax.ShapeDtypeStruct((row_dev, fields, nlon), jnp.float32),
        compiler_params=pltpu.CompilerParams(vmem_limit_bytes=ROW_VMEM),
        cost_estimate=pl.CostEstimate(flops=10**10, bytes_accessed=10**6, transcendentals=0),
        name="rows",
    )(row_length, *parts, pairs)


def rows_adjoint(grad_grid, kinds, share, pairs, row_length, trunc):
    count, fields, nlon = grad_grid.shape
    lanes = LANES * len(kinds)
    blocks = nlon // 2 // BLOCK
    tables, lefts = row_scratch(blocks, fields, lanes, nlon, BLOCK)
    span = blocks * BLOCK + LANES
    shapes = [(fields * 4 * count * (2 if kind == "own" else 1), LANES) for kind in kinds]
    return pl.pallas_call(
        lambda *refs: adjoint_kernel(kinds, share, trunc, grad_grid.shape, *refs),
        grid_spec=pltpu.PrefetchScalarGridSpec(
            num_scalar_prefetch=1,
            grid=(1,),
            in_specs=[pl.BlockSpec(memory_space=pltpu.HBM), pl.BlockSpec(memory_space=pltpu.VMEM)],
            out_specs=[pl.BlockSpec(memory_space=pltpu.VMEM)] * len(shapes),
            scratch_shapes=[
                pltpu.VMEM((count, fields, nlon // 2 + span), jnp.float32),
                pltpu.SemaphoreType.DMA((count,)),
                pair_scratch(pairs),
            ]
            + tables
            + lefts,
        ),
        out_shape=[jax.ShapeDtypeStruct(s, jnp.float32) for s in shapes],
        compiler_params=pltpu.CompilerParams(vmem_limit_bytes=ROW_VMEM),
        cost_estimate=pl.CostEstimate(flops=10**10, bytes_accessed=10**6, transcendentals=0),
        name="adjoint",
    )(row_length, grad_grid, pairs)


def body(spectrum, grad_grid, row_length, pair_of_slot):
    row_dev, grid_fields, nlon = grad_grid.shape
    own_fields, share, _, slots = spectrum.shape
    trunc = slots - 2
    lat = lax.axis_size("lat")
    wave = lax.axis_size("wave")
    wave_index = lax.axis_index("wave")
    combos = own_fields * 2
    total = pair_of_slot.shape[0]
    pairs = pair_of_slot[None, :]
    two = wave == 2
    swap = [(0, 1), (1, 0)]
    tiles = tuple(range(-(-total // LANES)))

    coeffs, table = synthesis(spectrum, pairs, row_dev * lat)
    coeffs = lax.all_to_all(coeffs, "lat", split_axis=0, concat_axis=0, tiled=True)

    if two:
        sent = rows_adjoint(grad_grid, ("other",), share, pairs, row_length, trunc)[0]
        received = lax.ppermute(sent, "wave", swap)
        kept = rows_adjoint(grad_grid, ("own",), share, pairs, row_length, trunc)[0]
        coeffs, kept = lax.optimization_barrier((coeffs, kept))
        grads = lax.dynamic_update_slice_in_dim(kept, received, (1 - wave_index) * received.shape[0], 0)
    else:
        folded = rows_adjoint(grad_grid, tiles, share, pairs, row_length, trunc)
        turned = jnp.concatenate(folded, axis=1)[:, :total].reshape(-1, wave, share)
        turned = jnp.pad(jnp.transpose(turned, (1, 0, 2)), ((0, 0), (0, 0), (0, LANES - share)))
        grads = lax.all_to_all(turned, "wave", split_axis=0, concat_axis=0, tiled=True)
    grads = grads.reshape(lat, combos * 2, row_dev, LANES)
    grads = lax.all_to_all(grads, "lat", split_axis=0, concat_axis=0, tiled=True)

    kinds = ("own", "other") if two else tiles
    if two:
        outgoing = lax.dynamic_slice_in_dim(coeffs, (1 - wave_index) * (lat // 2), lat // 2)
        parts = [coeffs, lax.ppermute(outgoing, "wave", swap)]
    else:
        turned = lax.all_to_all(coeffs, "wave", split_axis=0, concat_axis=0, tiled=True)
        turned = turned.reshape(wave, -1, LANES)[:, :, :share]
        turned = jnp.transpose(turned, (1, 0, 2)).reshape(turned.shape[1], -1)
        turned = jnp.pad(turned, ((0, 0), (0, LANES * len(tiles) - total)))
        parts = [turned[:, k * LANES : (k + 1) * LANES] for k in tiles]
    grid_field = rows_out(parts, kinds, share, pairs, row_length, grid_fields, nlon, trunc)

    grads, grid_field = lax.optimization_barrier((grads, grid_field))
    return grid_field, truncation(grads, pairs, table, spectrum.shape)


def solution(mesh):
    placed = (P("lat", "wave", None, None), P("lat", "wave", None), P("lat"), P())
    return jax.shard_map(
        body,
        mesh=mesh,
        in_specs=placed,
        out_specs=(P("lat", "wave", None), P("lat", "wave", None, None)),
        check_vma=False,
    )
```

```python
import math

import jax
import jax.numpy as jnp
import numpy as np
from jax import lax
from jax.experimental import pallas as pl
from jax.experimental.pallas import tpu as pltpu
from jax.sharding import PartitionSpec as P

GRID_LATS = 2560
LANES = 128
BLOCK = 256
SUB = 16
CHUNK = 8
GROUP = 2
AHEAD = 17
SYNTHESIS_VMEM = 56 * 1024 * 1024
TRUNCATION_VMEM = 52 * 1024 * 1024
ROW_VMEM = 20 * 1024 * 1024


def fit_trig():
    nodes = np.cos(np.pi * (np.arange(400) + 0.5) / 400)
    y = 0.125 * (nodes + 1.0) * 1.01
    u = np.sqrt(y)
    sin_fit = np.polynomial.chebyshev.Chebyshev.fit(y, np.sin(2 * np.pi * u) / u, 7, domain=[0, 0.2525])
    cos_fit = np.polynomial.chebyshev.Chebyshev.fit(y, np.cos(2 * np.pi * u), 8, domain=[0, 0.2525])
    to_power = lambda fit: [float(c) for c in fit.convert(kind=np.polynomial.Polynomial).coef]
    return to_power(sin_fit), to_power(cos_fit)


SIN_COEF, COS_COEF = fit_trig()


def horner(coefs, y):
    value = jnp.full_like(y, coefs[-1])
    for c in coefs[-2::-1]:
        value = value * y + c
    return value


def cos_sin(product, length, inverse):
    turns = jnp.floor(product * inverse + 0.5)
    u = (product - turns * length) * inverse
    y = u * u
    return horner(COS_COEF, y), u * horner(SIN_COEF, y)


def split(value):
    high = value.astype(jnp.bfloat16)
    low = (value - high.astype(jnp.float32)).astype(jnp.bfloat16)
    return high, low


def lane_pairs(pairs_ref, wide_ref, kind, share):
    total = pairs_ref.shape[1]
    width = wide_ref.shape[1]
    if kind in ("own", "other"):
        wave = lax.axis_index("wave")
        first = share * (wave if kind == "own" else 1 - wave)
        valid = share
    else:
        first = LANES * kind
        valid = min(LANES, total - first)
    wide_ref[0:1, :total] = pairs_ref[...]
    lanes = pltpu.roll(wide_ref[...], (width - first) % width, 1)[0:1, :LANES]
    return jnp.where(lax.broadcasted_iota(jnp.int32, (1, LANES), 1) < valid, lanes, 0)


def lane_facts(pairs_ref, wide_ref, share, trunc):
    pair = lane_pairs(pairs_ref, wide_ref, "own", share)
    boundary = trunc + 1 - pair
    delay = jnp.bitwise_and(-boundary, CHUNK - 1)
    return pair, delay, boundary + delay


def fill_coefficients(pair, delay, change, trunc, forward_ref, backward_ref):
    low_order = pair.astype(jnp.float32)
    high_order = trunc - low_order

    def fill(chunk, carry):
        step = lax.broadcasted_iota(jnp.int32, (CHUNK, LANES), 0) + chunk * CHUNK
        upper = step >= change
        order = jnp.where(upper, high_order, low_order)
        offset = jnp.where(upper, step - change, step - delay)
        degree = order + offset.astype(jnp.float32)
        lower = degree - 1.0
        top = jnp.maximum(4.0 * degree * degree - 1.0, 1.0)
        base = jnp.maximum(degree * degree - order * order, 1.0)
        lower_top = jnp.maximum(4.0 * lower * lower - 1.0, 1.0)
        lower_base = jnp.maximum(lower * lower - order * order, 1.0)
        forward = jnp.sqrt(top / base)
        backward = jnp.sqrt((top * lower_base) / (base * lower_top))
        rows = pl.ds(pl.multiple_of(chunk * CHUNK, CHUNK), CHUNK)
        forward_ref[rows, :] = jnp.where(offset <= 0, 0.0, forward)
        backward_ref[rows, :] = jnp.where(offset <= 0, -1.0, jnp.where(offset == 1, 0.0, backward))
        return carry

    lax.fori_loop(0, forward_ref.shape[0] // CHUNK, fill, 0, unroll=3)


def fill_starts(pair, trunc, geometry_ref, start_ref):
    rows = geometry_ref.shape[0]
    scales = []
    for order in (pair, trunc - pair):
        m = order.astype(jnp.float32)
        w = m + 8.75
        inverse = 1.0 / (w * w)
        ratio = jnp.sqrt(w) * (1.0 + inverse * (1.0 / 64.0 - (19.0 / 8192.0) * inverse))
        above = below = 1.0
        for k in range(1, 9):
            above = above * ((m + k) * (1.0 / 128.0))
            below = below * ((m + (k + 0.5)) * (1.0 / 128.0))
        scales.append((m, jnp.sqrt(ratio * above / (below * math.gamma(1.5)))))
    for first in range(0, rows, 8):
        row = lax.broadcasted_iota(jnp.int32, (8, LANES), 0) + first
        place = (2 * row + 1 - 2 * rows).astype(jnp.float32)
        _, sine = cos_sin(place, 4.0 * GRID_LATS, 0.25 / GRID_LATS)
        geometry_ref[first : first + 8, :] = -sine
        y = sine * sine
        series = jnp.full_like(y, 1.0 / 9.0)
        for k in range(8, 0, -1):
            series = series * y + 1.0 / k
        log_sine = -0.5 * y * series
        for k, (m, scale) in enumerate(scales):
            start_ref[k, first : first + 8, :] = scale * jnp.exp(m * log_sine)


def delayed(source_ref, start, delay, direction):
    options = [source_ref[pl.ds(start + direction * k, CHUNK), :] for k in range(CHUNK)]
    bit = 1
    while len(options) > 1:
        chosen = jnp.bitwise_and(delay, bit) != 0
        options = [jnp.where(chosen, options[k + 1], options[k]) for k in range(0, len(options), 2)]
        bit *= 2
    return options[0]


def legendre_step(t, latest, earlier, forward_ref, backward_ref, cosines):
    forward = forward_ref[pl.ds(t, 1), :]
    backward = backward_ref[pl.ds(t, 1), :]
    return [(forward * x) * v - backward * w for x, v, w in zip(cosines, latest, earlier)]


def first_change(trunc, pairs_total):
    least = trunc + 2 - pairs_total
    return -(-least // CHUNK)


def synthesis_kernel(
    remote_ref, pairs_ref, final_ref, table_ref, spectrum_ref, near_ref, out_ref, done_ref, block_ref, raw_ref, moved_ref,
    kept_ref, sent_ref, forward_ref, backward_ref, start_ref, geometry_ref, wide_ref,
):
    local = pltpu.make_async_copy(remote_ref, spectrum_ref, near_ref)
    local.start()
    share, parts, slots = spectrum_ref.shape[1:]
    trunc = slots - 2
    combos = out_ref.shape[1]
    half = out_ref.shape[0] // 2
    steps = forward_ref.shape[0]
    chunks = steps // CHUNK
    head = first_change(trunc, pairs_ref.shape[1])
    pair, delay, change = lane_facts(pairs_ref, wide_ref, share, trunc)
    fill_coefficients(pair, delay, change, trunc, forward_ref, backward_ref)
    fill_starts(pair, trunc, geometry_ref, start_ref)
    block_ref[...] = jnp.zeros_like(block_ref)
    local.wait()
    for j in range(combos):
        source = raw_ref.at[j]
        source[:CHUNK, :] = jnp.zeros((CHUNK, LANES), jnp.float32)
        for k in range(0, slots, LANES):
            width = min(LANES, slots - k)
            tile = block_ref.at[j, k // LANES]
            tile[:share, :width] = spectrum_ref[j // parts, :, j % parts, k : k + width]
            source[pl.ds(CHUNK + k, LANES), :] = tile[...].T

        def move(chunk, carry):
            start = pl.multiple_of(chunk * CHUNK, CHUNK)
            moved_ref[j, pl.ds(start, CHUNK), :] = delayed(source, start + CHUNK, delay, -1)
            return carry

        lax.fori_loop(0, chunks, move, 0, unroll=3)
    sign = jnp.where(delay % 2 == 0, 1.0, -1.0)

    def one_group(step, carry):
        del carry
        index = [step * GROUP + k for k in range(GROUP)]
        rows = [pl.ds(pl.multiple_of(g * 8, 8), 8) for g in index]
        cosines = [geometry_ref[r, :] for r in rows]
        lows = [start_ref[0, r, :] for r in rows]
        blank = [jnp.zeros((8, LANES), jnp.float32)] * (combos * GROUP)

        def chunk_steps(start, latest, earlier, even, odd):
            even, odd = list(even), list(odd)
            for u in range(CHUNK):
                value = legendre_step(start + u, latest, earlier, forward_ref, backward_ref, cosines)
                earlier, latest = latest, value
                for g in range(GROUP):
                    kept_ref[step, start + u, g] = value[g]
                sums = even if u % 2 == 0 else odd
                for j in range(combos):
                    weight = moved_ref[j, pl.ds(start + u, 1), :]
                    for g in range(GROUP):
                        sums[j * GROUP + g] = sums[j * GROUP + g] + weight * value[g]
            return latest, earlier, even, odd

        def head_chunk(chunk, state):
            return chunk_steps(pl.multiple_of(chunk * CHUNK, CHUNK), *state)

        def tail_chunk(chunk, state):
            latest, earlier, even, odd, even_low, odd_low = state
            start = pl.multiple_of(chunk * CHUNK, CHUNK)
            now = change == start
            even_low = [jnp.where(now, a, b) for a, b in zip(even, even_low)]
            odd_low = [jnp.where(now, a, b) for a, b in zip(odd, odd_low)]
            earlier = [jnp.where(now, start_ref[1, r, :], v) for r, v in zip(rows, earlier)]
            return (*chunk_steps(start, latest, earlier, even, odd), even_low, odd_low)

        state = lax.fori_loop(0, head, head_chunk, (lows, lows, blank, blank))
        copy(step, 0).start()
        state = lax.fori_loop(head, chunks, tail_chunk, (*state, blank, blank))
        _, _, even, odd, even_low, odd_low = state
        for j in range(combos):
            for g in range(GROUP):
                k = j * GROUP + g
                mirror = 2 * half - 1 - index[g]
                out_ref[index[g], j, 0] = even_low[k] + odd_low[k]
                out_ref[mirror, j, 0] = sign * (even_low[k] - odd_low[k])
                even_high = even[k] - even_low[k]
                odd_high = odd[k] - odd_low[k]
                out_ref[index[g], j, 1] = even_high + odd_high
                out_ref[mirror, j, 1] = even_high - odd_high
        copy(step, 1).start()
        deliver(step, 0).start()
        deliver(step, 1).start()
        return 0

    def deliver(step, mirror):
        first = 2 * half - (step + 1) * GROUP if mirror else step * GROUP
        rows = pl.ds(first, GROUP)
        return pltpu.make_async_copy(out_ref.at[rows], final_ref.at[rows], done_ref.at[step, mirror])

    def copy(step, piece):
        rows = pl.ds(head * CHUNK, steps - head * CHUNK) if piece else pl.ds(0, head * CHUNK)
        return pltpu.make_async_copy(kept_ref.at[step, rows], table_ref.at[step, rows], sent_ref.at[step, piece])

    lax.fori_loop(0, half // GROUP, one_group, 0)
    for step in range(half // GROUP):
        copy(step, 0).wait()
        copy(step, 1).wait()
        deliver(step, 0).wait()
        deliver(step, 1).wait()


def sum_sublanes(values):
    row = lax.broadcasted_iota(jnp.int32, (8, LANES), 0)
    near = row < 4
    level = [
        jnp.where(near, values[s], values[s + 4])
        + pltpu.roll(jnp.where(near, values[s + 4], values[s]), 4, 0)
        for s in range(4)
    ]
    for width in (2, 1):
        near = jnp.bitwise_and(row, width) == 0
        level = [
            jnp.where(
                near,
                level[s] + pltpu.roll(level[s], 8 - width, 0),
                level[s + width] + pltpu.roll(level[s + width], width, 0),
            )
            for s in range(width)
        ]
    return level[0]


def truncation_kernel(
    packed, grad_ref, pairs_ref, table_ref, out_ref, block_ref, kept_ref, come_ref, field_ref, turned_ref, final_ref, wide_ref,
):
    share, parts, slots = out_ref.shape[1:]
    combos = out_ref.shape[0] * parts
    half = grad_ref.shape[0] // 2
    steps = kept_ref.shape[1]
    blocks = come_ref.shape[0]
    span = steps // blocks

    def copy(k):
        rows = pl.ds(k * span, span)
        return pltpu.make_async_copy(table_ref.at[:, rows], kept_ref.at[:, rows], come_ref.at[k])

    for k in range(min(AHEAD, blocks)):
        copy(k).start()
    _, delay, change = lane_facts(pairs_ref, wide_ref, share, slots - 2)
    sign = jnp.where(delay % 2 == 0, 1.0, -1.0)

    def rows_of(device, k):
        return unpack_lanes(lambda q: grad_ref[device, q], k, share if packed else LANES)

    def fold(g, carry):
        for j in range(combos):
            for c in range(2):
                here = rows_of(g, 2 * j + c)
                there = rows_of(2 * half - 1 - g, 2 * j + c)
                if c == 0:
                    there = sign * there
                field_ref[0, c, j, g] = here + there
                field_ref[1, c, j, g] = here - there
        return carry

    lax.fori_loop(0, half, fold, 0)

    def block_steps(k, carry):
        copy(k).wait()

        @pl.when(k + AHEAD < blocks)
        def _():
            copy(k + AHEAD).start()

        def chunk_steps(chunk, carry):
            start = pl.multiple_of(k * span + chunk * CHUNK, CHUNK)
            upper = change <= start
            sums = {}
            for parity in range(2):
                for j in range(combos):
                    fields = [
                        jnp.where(upper, field_ref[parity, 1, j, g], field_ref[parity, 0, j, g]) for g in range(half)
                    ]
                    for u in range(parity, CHUNK, 2):
                        terms = [fields[g] * kept_ref[g // GROUP, start + u, g % GROUP] for g in range(half)]
                        while len(terms) > 1:
                            terms = [x + y for x, y in zip(terms[::2], terms[1::2])] + terms[len(terms) & ~1 :]
                        sums[u, j] = terms[0]
            for j in range(combos):
                turned_ref[j, pl.ds(start, CHUNK), :] = sum_sublanes([sums[u, j] for u in range(CHUNK)])
            return carry

        return lax.fori_loop(0, span // CHUNK, chunk_steps, carry)

    lax.fori_loop(0, blocks, block_steps, 0)

    for j in range(combos):
        source = turned_ref.at[j]

        def move(chunk, carry):
            start = pl.multiple_of(chunk * CHUNK, CHUNK)
            final_ref[pl.ds(start, CHUNK), :] = delayed(source, start, delay, 1)
            return carry

        lax.fori_loop(0, steps // CHUNK, move, 0, unroll=3)
        for k in range(0, slots, LANES):
            width = min(LANES, slots - k)
            tile = block_ref.at[j, k // LANES]
            tile[...] = final_ref[pl.ds(k, LANES), :].T
            out_ref[j // parts, :, j % parts, k : k + width] = tile[:share, :width]


def step_count(slots):
    return (slots + 2 * (CHUNK - 1)) // CHUNK * CHUNK


def legendre_call(kernel, arrays, places, out_places, out_shapes, scratch, limit):
    space = {"v": pltpu.VMEM, "h": pltpu.HBM}
    return pl.pallas_call(
        kernel,
        in_specs=[pl.BlockSpec(memory_space=space[p]) for p in places],
        out_specs=[pl.BlockSpec(memory_space=space[p]) for p in out_places],
        out_shape=[jax.ShapeDtypeStruct(shape, jnp.float32) for shape in out_shapes],
        scratch_shapes=scratch,
        compiler_params=pltpu.CompilerParams(vmem_limit_bytes=limit),
        cost_estimate=pl.CostEstimate(flops=10**10, bytes_accessed=10**6, transcendentals=0),
    )(*arrays)


def f32_scratch(*shape):
    return pltpu.VMEM(shape + (LANES,), jnp.float32)


def synthesis(spectrum, pairs, window_rows):
    fields, _, parts, slots = spectrum.shape
    combos = fields * parts
    steps = step_count(slots)
    tiles = -(-slots // LANES)
    passes = window_rows // 2 // 8 // GROUP
    table = (passes, steps, GROUP, 8, LANES)
    scratch = [
        pltpu.VMEM(spectrum.shape, jnp.float32),
        pltpu.SemaphoreType.DMA(()),
        pltpu.VMEM((window_rows // 8, combos, 2, 8, LANES), jnp.float32),
        pltpu.SemaphoreType.DMA((passes, 2)),
        f32_scratch(combos, tiles, LANES),
        f32_scratch(combos, CHUNK + tiles * LANES),
        f32_scratch(combos, steps),
        pltpu.VMEM(table, jnp.float32),
        pltpu.SemaphoreType.DMA((passes, 2)),
        f32_scratch(steps),
        f32_scratch(steps),
        f32_scratch(2, window_rows // 2),
        f32_scratch(window_rows // 2),
        pair_scratch(pairs),
    ]
    shapes = [(window_rows // 8, combos, 2, 8, LANES), table]
    return legendre_call(synthesis_kernel, (spectrum, pairs), "hv", "hh", shapes, scratch, SYNTHESIS_VMEM)


def truncation(grad, pairs, table, shape, packed):
    slots = shape[3]
    lat = grad.shape[0]
    combos = shape[0] * shape[2]
    steps = table.shape[1]
    tiles = -(-slots // LANES)
    chunks = steps // CHUNK
    blocks = next(n for n in range(min(chunks, 20), 0, -1) if chunks % n == 0)
    scratch = [
        f32_scratch(combos, tiles, LANES),
        pltpu.VMEM(table.shape, jnp.float32),
        pltpu.SemaphoreType.DMA((blocks,)),
        f32_scratch(2, 2, combos, lat // 2, 8),
        f32_scratch(combos, steps + CHUNK),
        f32_scratch(tiles * LANES),
        pair_scratch(pairs),
    ]
    arrays = (grad, pairs, table)
    kernel = lambda *refs: truncation_kernel(packed, *refs)
    return legendre_call(kernel, arrays, "vvh", "v", [shape], scratch, TRUNCATION_VMEM)[0]


def wave_rows(pairs_ref, wide_ref, kinds, share, trunc):
    pair = [lane_pairs(pairs_ref, wide_ref, kind, share) for kind in kinds]
    pair = jnp.concatenate(pair, axis=1) if len(pair) > 1 else pair[0]
    is_even = pair % 2 == 0
    even = jnp.where(is_even, pair, trunc - pair)
    return is_even, even.astype(jnp.float32), (trunc - even).astype(jnp.float32)


def row_place(row):
    flip = lax.axis_index("lat") >= lax.axis_size("lat") // 2
    return jnp.where(flip, 7 - row, row)


def row_tables(even, odd, length, inverse, table_refs):
    lanes = even.shape[1]
    steps = lax.broadcasted_iota(jnp.int32, (SUB, lanes), 0).astype(jnp.float32)
    for number, high_ref, low_ref in ((even, *table_refs[:2]), (odd, *table_refs[2:])):
        near_cos, near_sin = cos_sin(steps * number, length, inverse)
        far_cos, far_sin = cos_sin(steps * (number * SUB), length, inverse)
        for a in range(BLOCK // SUB):
            turn_cos = far_cos[a : a + 1, :]
            turn_sin = far_sin[a : a + 1, :]
            rows = pl.ds(a * SUB, SUB)
            high, low = split(near_cos * turn_cos - near_sin * turn_sin)
            high_ref[rows, :lanes] = high
            low_ref[rows, :lanes] = low
            high, low = split(near_sin * turn_cos + near_cos * turn_sin)
            high_ref[rows, lanes:] = high
            low_ref[rows, lanes:] = low


def outer_turns(number, blocks, length, inverse):
    steps = lax.broadcasted_iota(jnp.int32, (SUB * -(-blocks // SUB), number.shape[1]), 0).astype(jnp.float32)
    return cos_sin(steps * (number * BLOCK), length, inverse)


def three_pass(left_high, left_low, right_high, right_low, dims):
    dot = lambda a, b: lax.dot_general(a, b, (dims, ((), ())), preferred_element_type=jnp.float32)
    return dot(left_high, right_high) + (dot(left_low, right_high) + dot(left_high, right_low))


def row_kernel(kinds, share, trunc, length_ref, *refs):
    parts = len(kinds)
    part_refs = refs[:parts]
    pairs_ref, out_ref = refs[parts : parts + 2]
    table_refs = refs[parts + 2 : parts + 6]
    left_refs = refs[parts + 6 : parts + 10]
    shift_ref, wide_ref, pair_ref = refs[parts + 10 :]
    fields, nlon = out_ref.shape[1:]
    blocks = nlon // 2 // BLOCK
    row = pl.program_id(0)
    source = row_place(row)
    size = length_ref[row]
    half = size // 2
    length = size.astype(jnp.float32)
    inverse = 1.0 / jnp.full((1, LANES), length)[:, :1]
    is_even, even, odd = wave_rows(pairs_ref, pair_ref, kinds, share, trunc)
    row_tables(even, odd, length, inverse, table_refs)

    def coefficients(r, c):
        pieces = []
        for kind, ref in zip(kinds, part_refs):
            first = (r * 2 + c) * 8 + source
            if kind == "own":
                first = first + lax.axis_index("wave") * (fields * 32)
            pieces.append(ref[pl.ds(first, fields, stride=32), :])
        return jnp.concatenate(pieces, axis=1) if len(pieces) > 1 else pieces[0]

    lanes = even.shape[1]
    member = [[coefficients(r, c) for c in range(2)] for r in range(2)]
    for parity, number in ((0, even), (1, odd)):
        high_ref, low_ref = left_refs[2 * parity : 2 * parity + 2]
        weight = jnp.where(number == 0.0, 1.0, 2.0)
        real, imag = [
            jnp.where(is_even, member[r][parity], member[r][1 - parity]) * weight for r in range(2)
        ]
        turn_cos, turn_sin = outer_turns(number, blocks, length, inverse)
        for b in range(blocks):
            c = turn_cos[b : b + 1, :]
            s = turn_sin[b : b + 1, :]
            rows = pl.ds(b * fields, fields)
            high, low = split(real * c - imag * s)
            high_ref[rows, :lanes] = high
            low_ref[rows, :lanes] = low
            high, low = split(-(real * s + imag * c))
            high_ref[rows, lanes:] = high
            low_ref[rows, lanes:] = low

    dims = ((1,), (1,))
    even_sum = three_pass(left_refs[0][...], left_refs[1][...], table_refs[0][...], table_refs[1][...], dims)
    odd_sum = three_pass(left_refs[2][...], left_refs[3][...], table_refs[2][...], table_refs[3][...], dims)
    first = even_sum + odd_sum
    second = even_sum - odd_sum
    point = lax.broadcasted_iota(jnp.int32, (fields, BLOCK), 1)
    wide_ref[:, blocks * BLOCK :] = jnp.zeros((fields, wide_ref.shape[1] - blocks * BLOCK), jnp.float32)
    shift_ref[:, blocks * BLOCK :] = jnp.zeros((fields, LANES), jnp.float32)
    for b in range(blocks):
        inside = point < half - b * BLOCK
        cols = pl.ds(b * BLOCK, BLOCK)
        wide_ref[:, cols] = jnp.where(inside, first[b * fields : (b + 1) * fields], 0.0)
        shift_ref[:, cols] = jnp.where(inside, second[b * fields : (b + 1) * fields], 0.0)
    moved = pltpu.roll(shift_ref[...], half % LANES, 1)
    window = pl.ds(pl.multiple_of(half // LANES * LANES, LANES), blocks * BLOCK + LANES)
    wide_ref[:, window] = wide_ref[:, window] + moved
    out_ref[0] = wide_ref[:, :nlon]


def pack_lanes(values, share):
    lane = lax.broadcasted_iota(jnp.int32, values[0].shape, 1)
    tiles = []
    for q in range(-(-len(values) * share // LANES)):
        tile = None
        for k, value in enumerate(values):
            start = k * share - q * LANES
            if start < LANES and start + share > 0:
                moved = pltpu.roll(value, start % LANES, 1)
                tile = moved if tile is None else jnp.where(lane < start, tile, moved)
        tiles.append(tile)
    return tiles


def unpack_lanes(tile_of, k, share):
    q, start = divmod(k * share, LANES)
    value = tile_of(q)
    value = pltpu.roll(value, LANES - start, 1) if start else value
    if start + share <= LANES:
        return value
    lane = lax.broadcasted_iota(jnp.int32, value.shape, 1)
    return jnp.where(lane < LANES - start, value, pltpu.roll(tile_of(q + 1), LANES - start, 1))


def adjoint_kernel(kinds, share, trunc, packs, length_ref, grad_ref, pairs_ref, *refs):
    refs = list(refs)
    part_refs = [refs.pop(0) for _ in kinds]
    pair_ref = refs.pop(0)
    table_refs = [refs.pop(0) for _ in range(4)]
    sum_refs = [refs.pop(0) for _ in kinds] if packs else part_refs
    count, fields, nlon = grad_ref.shape
    blocks = nlon // 2 // BLOCK
    left_refs, (wide_ref, come_ref) = refs[:4], refs[4:]

    def copy(place):
        target = wide_ref.at[place, :, pl.ds(0, nlon)]
        return pltpu.make_async_copy(grad_ref.at[row_place(place)], target, come_ref.at[place])

    for place in range(min(2, count)):
        copy(place).start()
    is_even, even, odd = wave_rows(pairs_ref, pair_ref, kinds, share, trunc)
    lanes = even.shape[1]
    span = blocks * BLOCK + LANES
    point = lax.broadcasted_iota(jnp.int32, (fields, BLOCK), 1)

    def fold_row(place, half):
        window = pl.ds(pl.multiple_of(half // LANES * LANES, LANES), span)
        moved = pltpu.roll(wide_ref[place, :, window], (span - half % LANES) % span, 1)
        for b in range(blocks):
            inside = point < half - b * BLOCK
            cols = slice(b * BLOCK, (b + 1) * BLOCK)
            rows = pl.ds(b * fields, fields)
            early = jnp.where(inside, wide_ref[place, :, cols], 0.0)
            late = jnp.where(inside, moved[:, cols], 0.0)
            left_refs[0][rows, :], left_refs[1][rows, :] = split(early + late)
            left_refs[2][rows, :], left_refs[3][rows, :] = split(early - late)

    def one_row(place, carry):
        size = length_ref[row_place(place)]
        length = size.astype(jnp.float32)
        inverse = 1.0 / jnp.full((1, LANES), length)[:, :1]
        row_tables(even, odd, length, inverse, table_refs)
        copy(place).wait()

        @pl.when(place + 2 < count)
        def _():
            copy(place + 2).start()

        fold_row(place, size // 2)
        dims = ((1,), (0,))
        result = []
        for parity, number in ((0, even), (1, odd)):
            k = 2 * parity
            folded = three_pass(
                left_refs[k][...], left_refs[k + 1][...], table_refs[k][...], table_refs[k + 1][...], dims
            )
            turn_cos, turn_sin = outer_turns(number, blocks, length, inverse)
            real = imag = 0.0
            for b in range(blocks):
                c = turn_cos[b : b + 1, :]
                s = turn_sin[b : b + 1, :]
                cos_part = folded[b * fields : (b + 1) * fields, :lanes]
                sin_part = folded[b * fields : (b + 1) * fields, lanes:]
                real = real + (c * cos_part - s * sin_part)
                imag = imag - (s * cos_part + c * sin_part)
            weight = jnp.where(number == 0.0, 1.0, 2.0)
            result.append((weight * real, weight * imag))
        for r in range(2):
            for c in range(2):
                value = jnp.where(is_even, result[c][r], result[1 - c][r])
                for k, ref in enumerate(sum_refs):
                    rows = pl.ds((r * 2 + c) * count + place, fields, stride=4 * count)
                    ref[rows, :] = value[:, k * LANES : (k + 1) * LANES]
        return carry

    lax.fori_loop(0, count, one_row, 0)
    for kind, ref, sum_ref in zip(kinds, part_refs, sum_refs) if packs else ():
        values = 2 * 4
        chunks = fields * 4 // values

        def pack(chunk, carry):
            rows = [pl.ds(pl.multiple_of((chunk * values + k) * count, count), count) for k in range(values)]
            for q, tile in enumerate(pack_lanes([sum_ref[r, :] for r in rows], share)):
                ref[chunk, q] = tile
            return carry

        lax.fori_loop(0, chunks, pack, 0, unroll=4)


def row_scratch(blocks, fields, lanes, left_width):
    bf16 = jnp.bfloat16
    tables = [pltpu.VMEM((BLOCK, 2 * lanes), bf16)] * 4
    lefts = [pltpu.VMEM((blocks * fields, left_width), bf16)] * 4
    return tables, lefts


def pair_scratch(pairs):
    return pltpu.VMEM((8, -(-pairs.shape[1] // LANES) * LANES), jnp.int32)


def rows_out(parts, kinds, share, pairs, row_length, fields, nlon, trunc):
    row_dev = row_length.shape[0]
    lanes = LANES * len(kinds)
    blocks = nlon // 2 // BLOCK
    tables, lefts = row_scratch(blocks, fields, lanes, 2 * lanes)
    parts = [p.reshape(-1, LANES) for p in parts]
    span = blocks * BLOCK + LANES
    return pl.pallas_call(
        lambda *refs: row_kernel(kinds, share, trunc, *refs),
        grid_spec=pltpu.PrefetchScalarGridSpec(
            num_scalar_prefetch=1,
            grid=(row_dev,),
            in_specs=[pl.BlockSpec(memory_space=pltpu.VMEM)] * (len(parts) + 1),
            out_specs=pl.BlockSpec((1, fields, nlon), lambda i, *_: (i, 0, 0)),
            scratch_shapes=tables
            + lefts
            + [
                pltpu.VMEM((fields, span), jnp.float32),
                pltpu.VMEM((fields, nlon // 2 + span), jnp.float32),
                pair_scratch(pairs),
            ],
        ),
        out_shape=jax.ShapeDtypeStruct((row_dev, fields, nlon), jnp.float32),
        compiler_params=pltpu.CompilerParams(vmem_limit_bytes=ROW_VMEM),
        cost_estimate=pl.CostEstimate(flops=10**10, bytes_accessed=10**6, transcendentals=0),
        name="rows",
    )(row_length, *parts, pairs)


def rows_adjoint(grad_grid, kinds, share, pairs, row_length, trunc, packs):
    count, fields, nlon = grad_grid.shape
    lanes = LANES * len(kinds)
    blocks = nlon // 2 // BLOCK
    tables, lefts = row_scratch(blocks, fields, lanes, BLOCK)
    span = blocks * BLOCK + LANES
    flat = (fields * 4 * count, LANES)
    shapes = []
    for kind in kinds:
        if packs:
            shapes.append((fields // 2, -(-8 * share // LANES), count, LANES))
        else:
            shapes.append(flat)
    shapes = [jax.ShapeDtypeStruct(s, jnp.float32) for s in shapes]
    vmem = pl.BlockSpec(memory_space=pltpu.VMEM)
    scratch = [pair_scratch(pairs)] + tables
    if packs:
        scratch += [pltpu.VMEM(flat, jnp.float32) for _ in kinds]
    scratch += lefts
    scratch += [pltpu.VMEM((count, fields, nlon // 2 + span), jnp.float32), pltpu.SemaphoreType.DMA((count,))]
    return pl.pallas_call(
        lambda *refs: adjoint_kernel(kinds, share, trunc, packs, *refs),
        grid_spec=pltpu.PrefetchScalarGridSpec(
            num_scalar_prefetch=1,
            grid=(1,),
            in_specs=[pl.BlockSpec(memory_space=pltpu.HBM), vmem],
            out_specs=[vmem] * len(shapes),
            scratch_shapes=scratch,
        ),
        out_shape=shapes,
        compiler_params=pltpu.CompilerParams(vmem_limit_bytes=ROW_VMEM),
        cost_estimate=pl.CostEstimate(flops=10**10, bytes_accessed=10**6, transcendentals=0),
        name="adjoint",
    )(row_length, grad_grid, pairs)


def join_halves(mine, received):
    height = mine.shape[0]

    def kernel(mine_ref, received_ref, out_ref):
        wave = lax.axis_index("wave")
        out_ref[pl.ds(wave * height, height)] = mine_ref[...]
        out_ref[pl.ds((1 - wave) * height, height)] = received_ref[...]

    vmem = pl.BlockSpec(memory_space=pltpu.VMEM)
    return pl.pallas_call(
        kernel,
        in_specs=[vmem, vmem],
        out_specs=vmem,
        out_shape=jax.ShapeDtypeStruct((2 * height,) + mine.shape[1:], jnp.float32),
        compiler_params=pltpu.CompilerParams(vmem_limit_bytes=ROW_VMEM),
        name="join_halves",
    )(mine, received)


def body(spectrum, grad_grid, row_length, pair_of_slot):
    row_dev, grid_fields, nlon = grad_grid.shape
    own_fields, share, _, slots = spectrum.shape
    trunc = slots - 2
    lat = lax.axis_size("lat")
    wave = lax.axis_size("wave")
    wave_index = lax.axis_index("wave")
    combos = own_fields * 2
    total = pair_of_slot.shape[0]
    pairs = pair_of_slot[None, :]
    two = wave == 2
    swap = [(0, 1), (1, 0)]
    tiles = tuple(range(-(-total // LANES)))

    coeffs, table = synthesis(spectrum, pairs, row_dev * lat)
    coeffs = lax.all_to_all(coeffs, "lat", split_axis=0, concat_axis=0, tiled=True)

    if two:
        sent = rows_adjoint(grad_grid, ("other",), share, pairs, row_length, trunc, True)[0]
        received = lax.ppermute(sent, "wave", swap)
        kept = rows_adjoint(grad_grid, ("own",), share, pairs, row_length, trunc, True)[0]
        coeffs, kept = lax.optimization_barrier((coeffs, kept))
        grads = join_halves(kept, received)
    else:
        folded = rows_adjoint(grad_grid, tiles, share, pairs, row_length, trunc, False)
        turned = jnp.concatenate(folded, axis=1)[:, :total].reshape(-1, wave, share)
        turned = jnp.pad(jnp.transpose(turned, (1, 0, 2)), ((0, 0), (0, 0), (0, LANES - share)))
        grads = lax.all_to_all(turned, "wave", split_axis=0, concat_axis=0, tiled=True)
        grads = grads.reshape(lat, combos * 2, row_dev, LANES)
    grads = lax.all_to_all(grads, "lat", split_axis=0, concat_axis=0, tiled=True)

    kinds = ("own", "other") if two else tiles
    if two:
        outgoing = lax.dynamic_slice_in_dim(coeffs, (1 - wave_index) * (lat // 2), lat // 2)
        parts = [coeffs, lax.ppermute(outgoing, "wave", swap)]
    else:
        turned = lax.all_to_all(coeffs, "wave", split_axis=0, concat_axis=0, tiled=True)
        turned = turned.reshape(wave, -1, LANES)[:, :, :share]
        turned = jnp.transpose(turned, (1, 0, 2)).reshape(turned.shape[1], -1)
        turned = jnp.pad(turned, ((0, 0), (0, LANES * len(tiles) - total)))
        parts = [turned[:, k * LANES : (k + 1) * LANES] for k in tiles]
    grid_field = rows_out(parts, kinds, share, pairs, row_length, grid_fields, nlon, trunc)

    grads, grid_field = lax.optimization_barrier((grads, grid_field))
    return grid_field, truncation(grads, pairs, table, spectrum.shape, two)


def solution(mesh):
    placed = (P("lat", "wave", None, None), P("lat", "wave", None), P("lat"), P())
    return jax.shard_map(
        body,
        mesh=mesh,
        in_specs=placed,
        out_specs=(P("lat", "wave", None), P("lat", "wave", None, None)),
        check_vma=False,
    )
```
